32 devices in a mesh: gx: 4 (over z), gy: 2 (over y), gz: 4 (over x, core).
Axes of the slice: x: 2, y: 2, z: 4, core: 2. Of those that a mesh axis runs over, the one named last changes fastest.
Arguments:
- iterate: float32 [32, 32, 512], P('gx', 'gy', 'gz'), may hold values from -6 to 6
- source: float32 [32, 32, 512], P('gx', 'gy', 'gz'), may hold values from -6 to 6
- reaction: float32 [32, 32, 512], P('gx', 'gy', 'gz'), may hold values from 0.05 to 1
- trial_powers: int32 [4], replicated, may hold values from 0 to 5
Outputs:
- newton_dir: float32 [32, 32, 512], P('gx', 'gy', 'gz')
- remnant: float32 [32, 32, 512], P('gx', 'gy', 'gz')
- layer_energies: float32 [4, 32], P(None, 'gx')
- energies: float32 [4], replicated
The draws below stay inside these ranges and needn't reach their ends.
Inputs may be any that keep to these rules, and one draw needn't show every extreme that they name: `trial_powers`: trial k takes the step length 2 to the power minus entry k.
All inputs are finite; a program needn't handle non-finite values.
Results may differ from the reference program's by a relative error of at most 0.0003.
Values sent between devices are 32-bit elements; how exact they have to be, the bound alone decides.
A program may use at most 128 MiB of HBM per device.

```python
import math
import jax
import jax.numpy as jnp
from jax import lax

ITERS = 4
LEVELS = 4
TRIALS = 4
NX = 32
NY = 32
NZ = 512


def place_ends(array, rng, smallest, high):
    longest = array.shape.index(max(array.shape))
    spots = []
    for shift in (0, 1):
        where = [jax.random.randint(jax.random.fold_in(rng, axis), (), 0, length) for axis, length in enumerate(array.shape)]
        where[longest] = (where[longest] + shift) % array.shape[longest]
        spots.append(tuple(where))
    return array.at[spots[0]].set(smallest).at[spots[1]].set(high)


def level_of(key, extent, split, smallest, largest):
    def one(axis_at, shards_of):
        draws = jax.random.uniform(jax.random.fold_in(jax.random.fold_in(key, 6), axis_at), (shards_of,), jnp.float32, smallest / len(split), largest / len(split))
        return jnp.repeat(jnp.exp(draws), extent[axis_at] // shards_of).reshape((-1,) + (1,) * (len(extent) - axis_at - 1))

    loudness = one(*split[0])
    for cut in split[1:]:
        loudness = loudness * one(*cut)
    return loudness


def noise(rng, shape, spread, limit, split=(), kind=jnp.bfloat16):
    loudness = level_of(rng, shape, split, -0.22, 0.18) if split else 1.0
    entries = jax.random.normal(rng, shape, jnp.float32) * spread * loudness
    return jnp.minimum(jnp.maximum(entries, -limit), limit).astype(kind)


def setup_inputs(seed: int = 0) -> dict:
    key_list = jax.random.split(jax.random.key(seed), 5)
    return {
        "iterate": noise(key_list[0], (NX, NY, NZ), 1.0, 6.0, ((0, 4), (1, 2), (2, 4)), jnp.float32),
        "source": noise(key_list[1], (NX, NY, NZ), 1.0, 6.0, ((0, 4), (1, 2), (2, 4)), jnp.float32),
        "reaction": jnp.clip(jnp.exp(math.log(1.0) - 2.9957323 * jax.random.uniform(key_list[2], (NX, NY, NZ), jnp.float32) ** level_of(key_list[2], (NX, NY, NZ), ((0, 4), (1, 2), (2, 4)), -0.2, 0.2)), 0.05, 1.0),
        "trial_powers": place_ends(jax.random.randint(key_list[3], (TRIALS,), 0, 6), jax.random.fold_in(key_list[3], 1), 0, 5).astype(jnp.int32),
    }


cheb_mid = 1.15
cheb_half = 0.85

def differences(padded):
    along_x = padded[1:, 1:-1, 1:-1] - padded[:-1, 1:-1, 1:-1]
    along_y = padded[1:-1, 1:, 1:-1] - padded[1:-1, :-1, 1:-1]
    along_z = padded[1:-1, 1:-1, 1:] - padded[1:-1, 1:-1, :-1]
    return (along_x, along_y, along_z)

def stiffness(gradient):
    square = gradient * gradient
    return (1.0 + 2.0 * square) / jnp.sqrt(1.0 + square)

def fluxes(gradient):
    return gradient * jnp.sqrt(1.0 + gradient * gradient)

def face_energy(gradient):
    square = 1.0 + gradient * gradient
    return (square * jnp.sqrt(square) - 1.0) / 3.0

def divergence(face_flows):
    return face_flows[0][1:] - face_flows[0][:-1] + (face_flows[1][:, 1:] - face_flows[1][:, :-1]) + (face_flows[2][:, :, 1:] - face_flows[2][:, :, :-1])

def apply_operator(padded, weights, reaction):
    centre = padded[1:-1, 1:-1, 1:-1]
    gradient = differences(padded)
    face_flows = tuple((w * s for w, s in zip(weights, gradient)))
    return reaction * centre - divergence(face_flows)

def diagonal_of(weights, reaction):
    weight_x, weight_y, weight_z = weights
    return reaction + weight_x[1:] + weight_x[:-1] + weight_y[:, 1:] + weight_y[:, :-1] + weight_z[:, :, 1:] + weight_z[:, :, :-1]

def smooth(remnant, inverse, degree, operate):
    cheb_sigma = cheb_mid / cheb_half
    cheb_rho = 1.0 / cheb_sigma
    update = inverse * remnant / cheb_mid
    summed = update
    for sweep_idx in range(1, degree):
        remnant = remnant - operate(update)
        cheb_next = 1.0 / (2.0 * cheb_sigma - cheb_rho)
        update = cheb_next * cheb_rho * update + 2.0 * cheb_next / cheb_half * inverse * remnant
        summed = summed + update
        cheb_rho = cheb_next
    return (summed, remnant, update)

def pair_sum(values, axis_pos):
    old_shape = values.shape
    new_shape = old_shape[:axis_pos] + (old_shape[axis_pos] // 2, 2) + old_shape[axis_pos + 1:]
    return lax.optimization_barrier(jnp.sum(values.reshape(new_shape), axis=axis_pos + 1))

def restrict(values):
    return pair_sum(pair_sum(pair_sum(values, 0), 1), 2)

def prolong(values):
    return jnp.repeat(jnp.repeat(jnp.repeat(values, 2, 0), 2, 1), 2, 2)

def coarsen(weights, reaction):
    weight_x, weight_y, weight_z = weights
    coarse_x = pair_sum(pair_sum(weight_x[::2], 1), 2)
    coarse_y = pair_sum(pair_sum(weight_y[:, ::2], 0), 2)
    coarse_z = pair_sum(pair_sum(weight_z[:, :, ::2], 0), 1)
    return ((coarse_x, coarse_y, coarse_z), restrict(reaction))

def build_levels(weights, reaction):
    levels = [(weights, reaction, 1.0 / diagonal_of(weights, reaction))]
    for level_idx in range(1, LEVELS):
        weights, reaction = coarsen(weights, reaction)
        levels.append((weights, reaction, 1.0 / diagonal_of(weights, reaction)))
    return levels

def vcycle(levels, level_depth, remnant):
    weights, reaction, inverse = levels[level_depth]

    def operate(values):
        return apply_operator(jnp.pad(values, 1), weights, reaction)
    if level_depth == len(levels) - 1:
        summed, _, _ = smooth(remnant, inverse, 3, operate)
        return summed
    summed, remnant, update = smooth(remnant, inverse, 2, operate)
    remnant = remnant - operate(update)
    correction = prolong(vcycle(levels, level_depth + 1, restrict(remnant)))
    summed = summed + correction
    remnant = remnant - operate(correction)
    smoothed, _, _ = smooth(remnant, inverse, 2, operate)
    return summed + smoothed

def reference(iterate, source, reaction, trial_powers):
    gradient = differences(jnp.pad(iterate, 1))
    weights = tuple((stiffness(s) for s in gradient))
    remnant = source - reaction * iterate + divergence(tuple((fluxes(s) for s in gradient)))
    levels = build_levels(weights, reaction)
    newton_dir = jnp.zeros_like(iterate)
    precond_out = vcycle(levels, 0, remnant)
    direction = precond_out
    precond_norm = jnp.sum(remnant * precond_out)
    for iter_idx in range(ITERS):
        image_dir = apply_operator(jnp.pad(direction, 1), weights, reaction)
        step_length = precond_norm / jnp.sum(direction * image_dir)
        newton_dir = newton_dir + step_length * direction
        remnant = remnant - step_length * image_dir
        if iter_idx + 1 < ITERS:
            precond_out = vcycle(levels, 0, remnant)
            norm_next = jnp.sum(remnant * precond_out)
            direction = precond_out + norm_next / precond_norm * direction
            precond_norm = norm_next
    layer_cells = NY * NZ
    layers = []
    for trial_idx in range(TRIALS):
        step_scale = jnp.exp2(-trial_powers[trial_idx].astype(jnp.float32))
        trial_field = iterate + step_scale * newton_dir
        trial_slopes = differences(jnp.pad(trial_field, 1))
        energy_x = face_energy(trial_slopes[0])
        layer_sum = lax.optimization_barrier(jnp.sum(energy_x[:-1], axis=(1, 2)))
        layer_sum = layer_sum.at[-1].add(jnp.sum(energy_x[-1]))
        layer_sum = layer_sum + lax.optimization_barrier(jnp.sum(face_energy(trial_slopes[1]), axis=(1, 2))) + lax.optimization_barrier(jnp.sum(face_energy(trial_slopes[2]), axis=(1, 2)))
        layer_sum = layer_sum + lax.optimization_barrier(jnp.sum(0.5 * reaction * trial_field * trial_field - source * trial_field, axis=(1, 2)))
        layers.append(layer_sum / layer_cells)
    layer_energies = jnp.stack(layers)
    energies = lax.optimization_barrier(jnp.sum(layer_energies, axis=1)) / NX
    return (newton_dir, remnant, layer_energies, energies)
```

```python
import functools

import jax
import jax.numpy as jnp
from jax import lax
from jax.experimental import pallas as pl
from jax.experimental.pallas import tpu as pltpu
from jax.sharding import PartitionSpec as P

ITERS = 4
LEVELS = 4
TRIALS = 4
MID = 1.15
HALF = 0.85
SIGMA = MID / HALF
RHO0 = 1.0 / SIGMA
RHO1 = 1.0 / (2.0 * SIGMA - RHO0)
RHO2 = 1.0 / (2.0 * SIGMA - RHO1)
ROUND = 3
KEPT = ROUND
DG, INV, XM, XP, YM, YP, ZM, ZP, YB, ZB = range(10)
MESH = pl.DeviceIdType.MESH


def kernel(
    sizes, counts, tp_ref, it_ref, src_ref, rea_ref, dir_ref, rem_ref, le_ref, en_ref,
    sx, rx, sy, ry, sz, rz, ssem, rsem, lev0, lev1, lev2, lev3, p_ref, q_ref,
    phx, phy, phz, dhx, dhy, dhz, dot_pl, dot_x, en_pl, en_x, red_ssem, red_rsem,
):
    X, Y, Z = sizes
    nx, ny, nz = counts
    planes = ny * nz
    levs = (lev0, lev1, lev2, lev3)
    ix, iy, iz = lax.axis_index("gx"), lax.axis_index("gy"), lax.axis_index("gz")
    has = (ix > 0, ix < nx - 1, iy > 0, iy < ny - 1, iz > 0, iz < nz - 1)
    devs = (
        (ix - 1, iy, iz), (ix + 1, iy, iz), (ix, iy - 1, iz),
        (ix, iy + 1, iz), (ix, iy, iz - 1), (ix, iy, iz + 1),
    )
    send = (sx, sx, sy, sy, sz, sz)
    recv = (rx, rx, ry, ry, rz, rz)
    lane_y = lax.broadcasted_iota(jnp.int32, (Y, Z), 1)
    lane_1 = lax.broadcasted_iota(jnp.int32, (1, Z), 1)

    def rows_of(x):
        return lax.rem(lax.broadcasted_iota(jnp.int32, (x * Y, Z), 0), Y)

    def lanes_of(x):
        return lax.broadcasted_iota(jnp.int32, (x * Y, Z), 1)

    def cat(parts):
        return parts[0] if len(parts) == 1 else jnp.concatenate(parts, axis=0)

    def roll(v, shift, axis):
        return pltpu.roll(v, shift % v.shape[axis], axis)

    for d in range(6):
        @pl.when(jnp.logical_not(has[d]))
        def _():
            recv[d][:, d % 2] = jnp.zeros(recv[d].shape[:1] + recv[d].shape[2:], jnp.float32)

    def outgoing(d, slot):
        side = d % 2
        return pltpu.make_async_remote_copy(
            src_ref=send[d].at[slot, side],
            dst_ref=recv[d].at[slot, 1 - side],
            send_sem=ssem.at[slot, d],
            recv_sem=rsem.at[slot, d + 1 - 2 * side],
            device_id=devs[d],
            device_id_type=MESH,
        )

    def incoming(d, slot):
        side = d % 2
        return pltpu.make_async_remote_copy(
            src_ref=send[d].at[slot, side],
            dst_ref=recv[d].at[slot, side],
            send_sem=ssem.at[slot, d],
            recv_sem=rsem.at[slot, d],
            device_id=devs[d],
            device_id_type=MESH,
        )

    def go(d, slot):
        @pl.when(has[d])
        def _():
            outgoing(d, slot).start()

    def start(v, slot):
        x = v.shape[0] // Y
        sx[slot, 0] = v[:Y]
        sx[slot, 1] = v[-Y:]
        go(0, slot)
        go(1, slot)
        for i in range(x):
            sy[slot, 0, i : i + 1] = v[i * Y : i * Y + 1]
            sy[slot, 1, i : i + 1] = v[i * Y + Y - 1 : i * Y + Y]
        go(2, slot)
        go(3, slot)
        for side, lane in ((0, 0), (1, Z - 1)):
            packed = jnp.broadcast_to(v[:Y, lane : lane + 1], (Y, Z))
            for i in range(1, x):
                part = jnp.broadcast_to(v[i * Y : i * Y + Y, lane : lane + 1], (Y, Z))
                packed = jnp.where(lane_y == i, part, packed)
            sz[slot, side] = packed
        go(4, slot)
        go(5, slot)

    def finish(slot):
        for d in range(6):
            @pl.when(has[d])
            def _():
                copy = incoming(d, slot)
                copy.wait_recv()
                copy.wait_send()

    def wide_y(half, x):
        return cat([jnp.broadcast_to(half[i : i + 1], (Y, Z)) for i in range(x)])

    def wide_z(half, x):
        return cat([jnp.broadcast_to(half[:, i : i + 1], (Y, Z)) for i in range(x)])

    def operate(v, level, slot):
        w = levs[level]
        step = 1 << level
        x = X >> level
        start(v, slot)
        acc = w[DG] * v
        acc = acc - w[YM] * roll(v, step, 0) - w[YP] * roll(v, -step, 0)
        acc = acc - w[ZM] * roll(v, step, 1) - w[ZP] * roll(v, -step, 1)
        if x > 1:
            none = jnp.zeros((Y, Z), jnp.float32)
            acc = acc - w[XM] * cat([none, v[:-Y]]) - w[XP] * cat([v[Y:], none])
        finish(slot)
        in_y = jnp.where(rows_of(x) < Y // 2, wide_y(ry[slot, 0], x), wide_y(ry[slot, 1], x))
        in_z = jnp.where(lanes_of(x) < Z // 2, wide_z(rz[slot, 0], x), wide_z(rz[slot, 1], x))
        acc = acc - w[YB] * in_y - w[ZB] * in_z
        low = w[XM, :Y] * rx[slot, 0]
        high = w[XP, (x - 1) * Y :] * rx[slot, 1]
        if x == 1:
            return acc - low - high
        parts = [acc[:Y] - low] + ([acc[Y:-Y]] if x > 2 else []) + [acc[-Y:] - high]
        return cat(parts)

    def pair_x(v):
        x = v.shape[0] // Y
        return cat([v[2 * i * Y : (2 * i + 1) * Y] + v[(2 * i + 1) * Y : (2 * i + 2) * Y] for i in range(x // 2)])

    def pick_x(v, odd):
        x = v.shape[0] // Y
        return cat([v[(2 * i + odd) * Y : (2 * i + odd + 1) * Y] for i in range(x // 2)])

    def bit(v, level, axis):
        at = rows_of(v.shape[0] // Y) if axis == 0 else lanes_of(v.shape[0] // Y)
        return lax.rem(at, 2 << level) < (1 << level)

    def pair(v, level, axis):
        step = 1 << level
        return v + jnp.where(bit(v, level, axis), roll(v, -step, axis), roll(v, step, axis))

    def pick(v, level, axis, odd):
        step = 1 << level
        low = bit(v, level, axis)
        if odd:
            return jnp.where(low, roll(v, -step, axis), v)
        return jnp.where(low, v, roll(v, step, axis))

    def restrict(v, level):
        return pair(pair(pair_x(v), level, 0), level, 1)

    def prolong(v):
        x = v.shape[0] // Y
        return cat([v[(i // 2) * Y : (i // 2 + 1) * Y] for i in range(2 * x)])

    def put_level(level, ws, reaction):
        xm, xp, ym, yp, zm, zp = ws
        w = levs[level]
        step = 1 << level
        x = X >> level
        rows, lanes = rows_of(x), lanes_of(x)
        diagonal = reaction + xm + xp + ym + yp + zm + zp
        zero = jnp.zeros_like(xm)
        w[DG] = diagonal
        w[INV] = 1.0 / diagonal
        w[XM] = xm
        w[XP] = xp
        w[YM] = jnp.where(rows < step, zero, ym)
        w[YP] = jnp.where(rows >= Y - step, zero, yp)
        w[ZM] = jnp.where(lanes < step, zero, zm)
        w[ZP] = jnp.where(lanes >= Z - step, zero, zp)
        w[YB] = jnp.where(rows < step, ym, jnp.where(rows >= Y - step, yp, zero))
        w[ZB] = jnp.where(lanes < step, zm, jnp.where(lanes >= Z - step, zp, zero))

    turn = [0]

    def apply(v, level):
        slot = turn[0] % ROUND
        turn[0] += 1
        return operate(v, level, slot)

    def vcycle(r, level):
        w = levs[level]
        u = w[INV] * r * (1.0 / MID)
        total = u
        r = r - apply(u, level)
        u = RHO1 * RHO0 * u + 2.0 * RHO1 / HALF * w[INV] * r
        total = total + u
        r = r - apply(u, level)
        if level == LEVELS - 1:
            u = RHO2 * RHO1 * u + 2.0 * RHO2 / HALF * w[INV] * r
            return total + u
        e = prolong(vcycle(restrict(r, level), level + 1))
        total = total + e
        r = r - apply(e, level)
        u = w[INV] * r * (1.0 / MID)
        total = total + u
        r = r - apply(u, level)
        u = RHO1 * RHO0 * u + 2.0 * RHO1 / HALF * w[INV] * r
        return total + u

    def gather(ref, part, count, me, device, which):
        for j in range(count):
            @pl.when(me != j)
            def _():
                pltpu.make_async_remote_copy(
                    src_ref=ref.at[part, me],
                    dst_ref=ref.at[part, me],
                    send_sem=red_ssem.at[which, part],
                    recv_sem=red_rsem.at[which, part],
                    device_id=device(j),
                    device_id_type=MESH,
                ).start()
        if count > 1:
            others = ref.at[part, pl.ds(0, count - 1)]
            pltpu.make_async_copy(others, others, red_rsem.at[which, part]).wait()
            pltpu.make_async_copy(others, others, red_ssem.at[which, part]).wait()

    def in_plane(j):
        return (ix, j // nz, j % nz)

    def in_column(j):
        return (j, iy, iz)

    my_plane = iy * nz + iz

    def reduce_plane(ref, part, value, which):
        ref[part, my_plane] = value
        gather(ref, part, planes, my_plane, in_plane, which)
        return jnp.sum(ref[part], axis=0)

    def reduce_column(ref, part, value, which):
        ref[part, ix] = value
        gather(ref, part, nx, ix, in_column, which)
        return jnp.sum(ref[part], axis=0)

    def total_of(v):
        return jnp.sum(jnp.sum(v, axis=0, keepdims=True), axis=1, keepdims=True)

    def lane_of(row, i):
        return jnp.sum(jnp.where(lane_1 == i, row, 0.0), axis=1, keepdims=True)

    it = it_ref[...].reshape(X * Y, Z)
    reaction = rea_ref[...].reshape(X * Y, Z)
    start(it, KEPT)
    finish(KEPT)
    rows, lanes = rows_of(X), lanes_of(X)
    last_row, last_lane = rows == Y - 1, lanes == Z - 1
    n_xm = cat([rx[KEPT, 0], it[:-Y]])
    n_xp = cat([it[Y:], rx[KEPT, 1]])
    n_ym = jnp.where(rows == 0, wide_y(ry[KEPT, 0], X), roll(it, 1, 0))
    n_yp = jnp.where(last_row, wide_y(ry[KEPT, 1], X), roll(it, -1, 0))
    n_zm = jnp.where(lanes == 0, wide_z(rz[KEPT, 0], X), roll(it, 1, 1))
    n_zp = jnp.where(last_lane, wide_z(rz[KEPT, 1], X), roll(it, -1, 1))
    ws = []
    r = src_ref[...].reshape(X * Y, Z) - reaction * it
    for sign, n in ((-1, n_xm), (1, n_xp), (-1, n_ym), (1, n_yp), (-1, n_zm), (1, n_zp)):
        g = n - it
        square = g * g
        root = jnp.sqrt(1.0 + square)
        ws.append((1.0 + 2.0 * square) / root)
        r = r + g * root
    rem_ref[...] = r.reshape(X, Y, Z)
    put_level(0, ws, reaction)
    for level in range(LEVELS - 1):
        xm, xp, ym, yp, zm, zp = ws
        ws = (
            pair(pair(pick_x(xm, 0), level, 0), level, 1),
            pair(pair(pick_x(xp, 1), level, 0), level, 1),
            pair(pick(pair_x(ym), level, 0, 0), level, 1),
            pair(pick(pair_x(yp), level, 0, 1), level, 1),
            pick(pair(pair_x(zm), level, 0), level, 1, 0),
            pick(pair(pair_x(zp), level, 0), level, 1, 1),
        )
        reaction = restrict(reaction, level)
        put_level(level + 1, ws, reaction)
    for ref in (p_ref, q_ref, phx, phy, phz, dhx, dhy, dhz):
        ref[...] = jnp.zeros_like(ref)
    dir_ref[...] = jnp.zeros_like(dir_ref)

    def body(it_idx, carry):
        rz_old, pq_old = carry
        part = lax.rem(it_idx, 2)
        r = rem_ref[...].reshape(X * Y, Z)
        turn[0] = 0
        z = vcycle(r, 0)
        z_slot = turn[0] % ROUND
        az = apply(z, 0)
        q_old = q_ref[...]
        sums = jnp.where(
            lane_1 == 0,
            total_of(rem_ref[...].reshape(X * Y, Z) * z),
            jnp.where(lane_1 == 1, total_of(z * az), total_of(z * q_old)),
        )
        row = reduce_plane(dot_pl, part, sums, 0)
        row = reduce_column(dot_x, part, row, 1)
        rz_new, zaz, zq = lane_of(row, 0), lane_of(row, 1), lane_of(row, 2)
        beta = rz_new / rz_old
        pq = zaz + 2.0 * beta * zq + beta * beta * pq_old
        a = rz_new / pq
        p = z + beta * p_ref[...]
        q = az + beta * q_old
        p_ref[...] = p
        q_ref[...] = q
        dir_ref[...] = dir_ref[...] + (a * p).reshape(X, Y, Z)
        rem_ref[...] = rem_ref[...] - (a * q).reshape(X, Y, Z)
        for got, ph, dh in ((rx, phx, dhx), (ry, phy, dhy), (rz, phz, dhz)):
            for side in range(2):
                edge = got[z_slot, side] + beta * ph[side]
                ph[side] = edge
                dh[side] = dh[side] + a * edge
        return rz_new, pq

    one = jnp.ones((1, 1), jnp.float32)
    lax.fori_loop(0, ITERS, body, (one, jnp.zeros((1, 1), jnp.float32)))

    it = it_ref[...].reshape(X * Y, Z)
    step_dir = dir_ref[...].reshape(X * Y, Z)

    def energy(g):
        square = 1.0 + g * g
        return (square * jnp.sqrt(square) - 1.0) * (1.0 / 3.0)

    ends_y = jnp.where(jnp.logical_and(last_row, iy == ny - 1), 1.0, 0.0)
    ends_z = jnp.where(jnp.logical_and(last_lane, iz == nz - 1), 1.0, 0.0)
    ends_x = jnp.where(ix == nx - 1, 1.0, 0.0)
    across = lax.broadcasted_iota(jnp.int32, (X, Z), 0) == lax.broadcasted_iota(jnp.int32, (X, Z), 1)
    trial_rows = []
    for k in range(TRIALS):
        s = jnp.exp2(-jnp.full((1, Z), tp_ref[k], jnp.int32).astype(jnp.float32))
        v = it + s * step_dir
        low_x = cat([rx[KEPT, 0] + s * dhx[0], v[:-Y]])
        low_y = jnp.where(rows == 0, wide_y(ry[KEPT, 0] + s * dhy[0], X), roll(v, 1, 0))
        low_z = jnp.where(lanes == 0, wide_z(rz[KEPT, 0] + s * dhz[0], X), roll(v, 1, 1))
        at_end = energy(v)
        e = energy(v - low_x) + energy(v - low_y) + energy(v - low_z)
        e = e + at_end * (ends_y + ends_z)
        e = cat([e[:-Y], e[-Y:] + ends_x * at_end[-Y:]]) if X > 1 else e + ends_x * at_end
        e = e + 0.5 * rea_ref[...].reshape(X * Y, Z) * v * v - src_ref[...].reshape(X * Y, Z) * v
        by_layer = jnp.sum(jnp.sum(e.reshape(X, Y, Z), axis=1), axis=1, keepdims=True)
        trial_rows.append(jnp.sum(jnp.where(across, by_layer, 0.0), axis=0, keepdims=True))
    layers = reduce_plane(en_pl, 0, jnp.concatenate(trial_rows, axis=0), 2)
    layers = layers / (Y * ny * Z * nz)
    le_ref[...] = layers[:, :X]
    overall = reduce_column(en_x, 0, layers, 3)
    overall = jnp.sum(overall, axis=1, keepdims=True) / (X * nx)
    en_ref[...] = jnp.broadcast_to(overall, (TRIALS, Z))


def on_device(counts, iterate, source, reaction, trial_powers):
    X, Y, Z = iterate.shape
    nx, ny, nz = counts
    f32 = jnp.float32
    slots = ROUND + 1
    vm = pltpu.VMEM
    scratch = [vm((slots, 2, rows, Z), f32) for rows in (Y, Y, X, X, Y, Y)]
    scratch += [pltpu.SemaphoreType.DMA((slots, 6))] * 2
    scratch += [vm((10, (X >> level) * Y, Z), f32) for level in range(LEVELS)]
    scratch += [vm((X * Y, Z), f32)] * 2
    scratch += [vm((2, rows, Z), f32) for rows in (Y, X, Y)] * 2
    scratch += [
        vm((2, ny * nz, 1, Z), f32), vm((2, nx, 1, Z), f32),
        vm((1, ny * nz, TRIALS, Z), f32), vm((1, nx, TRIALS, Z), f32),
        pltpu.SemaphoreType.DMA((4, 2)), pltpu.SemaphoreType.DMA((4, 2)),
    ]
    whole = pl.BlockSpec(memory_space=pltpu.VMEM)
    out = pl.pallas_call(
        functools.partial(kernel, (X, Y, Z), counts),
        out_shape=[
            jax.ShapeDtypeStruct((X, Y, Z), f32),
            jax.ShapeDtypeStruct((X, Y, Z), f32),
            jax.ShapeDtypeStruct((TRIALS, X), f32),
            jax.ShapeDtypeStruct((TRIALS, Z), f32),
        ],
        in_specs=[pl.BlockSpec(memory_space=pltpu.SMEM), whole, whole, whole],
        out_specs=[whole] * 4,
        scratch_shapes=scratch,
        compiler_params=pltpu.CompilerParams(has_side_effects=True, vmem_limit_bytes=48 * 1024 * 1024),
        name="newton_step",
    )(trial_powers, iterate, source, reaction)
    return out[0], out[1], out[2], out[3][:, 0]


def solution(mesh):
    counts = tuple(mesh.shape[axis] for axis in ("gx", "gy", "gz"))
    grid = P("gx", "gy", "gz")
    return jax.shard_map(
        functools.partial(on_device, counts),
        mesh=mesh,
        in_specs=(grid, grid, grid, P()),
        out_specs=(grid, grid, P(None, "gx"), P()),
        check_vma=False,
    )
```

```python
import functools

import jax
import jax.numpy as jnp
from jax import lax
from jax.experimental import pallas as pl
from jax.experimental.pallas import tpu as pltpu
from jax.sharding import PartitionSpec as P

ITERS = 4
LEVELS = 4
TRIALS = 4
MID = 1.15
HALF = 0.85
SIGMA = MID / HALF
RHO0 = 1.0 / SIGMA
RHO1 = 1.0 / (2.0 * SIGMA - RHO0)
RHO2 = 1.0 / (2.0 * SIGMA - RHO1)
ROUND = 3
KEPT = ROUND
DG, INV, XM, XP, YM, YP, ZM, ZP, YB, ZB = range(10)
MESH = pl.DeviceIdType.MESH


class Grid:
    def __init__(self, Y, Z):
        self.Y, self.Z = Y, Z

    def rows_of(self, x):
        return lax.rem(lax.broadcasted_iota(jnp.int32, (x * self.Y, self.Z), 0), self.Y)

    def lanes_of(self, x):
        return lax.broadcasted_iota(jnp.int32, (x * self.Y, self.Z), 1)

    def pair_x(self, v):
        Y = self.Y
        x = v.shape[0] // Y
        return cat([v[2 * i * Y : (2 * i + 1) * Y] + v[(2 * i + 1) * Y : (2 * i + 2) * Y] for i in range(x // 2)])

    def pick_x(self, v, odd):
        Y = self.Y
        x = v.shape[0] // Y
        return cat([v[(2 * i + odd) * Y : (2 * i + odd + 1) * Y] for i in range(x // 2)])

    def bit(self, v, level, axis):
        at = self.rows_of(v.shape[0] // self.Y) if axis == 0 else self.lanes_of(v.shape[0] // self.Y)
        return lax.rem(at, 2 << level) < (1 << level)

    def pair(self, v, level, axis):
        step = 1 << level
        return v + jnp.where(self.bit(v, level, axis), roll(v, -step, axis), roll(v, step, axis))

    def pick(self, v, level, axis, odd):
        step = 1 << level
        low = self.bit(v, level, axis)
        if odd:
            return jnp.where(low, roll(v, -step, axis), v)
        return jnp.where(low, v, roll(v, step, axis))

    def restrict(self, v, level):
        return self.pair(self.pair(self.pair_x(v), level, 0), level, 1)

    def prolong(self, v):
        Y = self.Y
        x = v.shape[0] // Y
        return cat([v[(i // 2) * Y : (i // 2 + 1) * Y] for i in range(2 * x)])

    def coarsen(self, ws, reaction, level):
        xm, xp, ym, yp, zm, zp = ws
        pair, pick = self.pair, self.pick
        ws = (
            pair(pair(self.pick_x(xm, 0), level, 0), level, 1),
            pair(pair(self.pick_x(xp, 1), level, 0), level, 1),
            pair(pick(self.pair_x(ym), level, 0, 0), level, 1),
            pair(pick(self.pair_x(yp), level, 0, 1), level, 1),
            pick(pair(self.pair_x(zm), level, 0), level, 1, 0),
            pick(pair(self.pair_x(zp), level, 0), level, 1, 1),
        )
        return ws, self.restrict(reaction, level)

    def put(self, w, level, ws, reaction):
        Y, Z = self.Y, self.Z
        xm, xp, ym, yp, zm, zp = ws
        step = 1 << level
        x = xm.shape[0] // Y
        rows, lanes = self.rows_of(x), self.lanes_of(x)
        diagonal = reaction + xm + xp + ym + yp + zm + zp
        zero = jnp.zeros_like(xm)
        w[DG] = diagonal
        w[INV] = 1.0 / diagonal
        w[XM] = xm
        w[XP] = xp
        w[YM] = jnp.where(rows < step, zero, ym)
        w[YP] = jnp.where(rows >= Y - step, zero, yp)
        w[ZM] = jnp.where(lanes < step, zero, zm)
        w[ZP] = jnp.where(lanes >= Z - step, zero, zp)
        if w.shape[0] > YB:
            w[YB] = jnp.where(rows < step, ym, jnp.where(rows >= Y - step, yp, zero))
            w[ZB] = jnp.where(lanes < step, zm, jnp.where(lanes >= Z - step, zp, zero))

    def inner(self, w, v, level):
        step = 1 << level
        acc = w[DG] * v
        acc = acc - w[YM] * roll(v, step, 0) - w[YP] * roll(v, -step, 0)
        acc = acc - w[ZM] * roll(v, step, 1) - w[ZP] * roll(v, -step, 1)
        Y = self.Y
        if v.shape[0] > Y:
            none = jnp.zeros((Y, self.Z), jnp.float32)
            acc = acc - w[XM] * cat([none, v[:-Y]]) - w[XP] * cat([v[Y:], none])
        return acc


def cat(parts):
    return parts[0] if len(parts) == 1 else jnp.concatenate(parts, axis=0)


def roll(v, shift, axis):
    return pltpu.roll(v, shift % v.shape[axis], axis)


def dot(a, b):
    return lax.dot_general(
        a, b, (((1,), (0,)), ((), ())), precision=lax.Precision.HIGHEST, preferred_element_type=jnp.float32
    )


def kernel(
    sizes, counts, tp_ref, it_ref, src_ref, rea_ref, dir_ref, rem_ref, le_ref, en_ref,
    sx, rx, sy, ry, sz, rz, ssem, rsem, lev0, lev1, glev2, glev3, p_ref, q_ref,
    phx, phy, phz, dhx, dhy, dhz, dot_pl, dot_x, en_pl, en_x, red_ssem, red_rsem,
    picked, gat_pl, gat_x, set_pl, set_x, glob,
):
    X, Y, Z = sizes
    nx, ny, nz = counts
    planes = ny * nz
    levs = (lev0, lev1)
    L = len(levs)
    x_own, y_own, z_own = X >> L, Y >> L, Z >> L
    GY, GZ = ny * y_own, nz * z_own
    here, world = Grid(Y, Z), Grid(GY, GZ)
    rows_of, lanes_of = here.rows_of, here.lanes_of
    ix, iy, iz = lax.axis_index("gx"), lax.axis_index("gy"), lax.axis_index("gz")
    has = (ix > 0, ix < nx - 1, iy > 0, iy < ny - 1, iz > 0, iz < nz - 1)
    devs = (
        (ix - 1, iy, iz), (ix + 1, iy, iz), (ix, iy - 1, iz),
        (ix, iy + 1, iz), (ix, iy, iz - 1), (ix, iy, iz + 1),
    )
    send = (sx, sx, sy, sy, sz, sz)
    recv = (rx, rx, ry, ry, rz, rz)
    lane_y = lax.broadcasted_iota(jnp.int32, (Y, Z), 1)
    lane_1 = lax.broadcasted_iota(jnp.int32, (1, Z), 1)

    for d in range(6):
        @pl.when(jnp.logical_not(has[d]))
        def _():
            recv[d][:, d % 2] = jnp.zeros(recv[d].shape[:1] + recv[d].shape[2:], jnp.float32)

    def outgoing(d, slot):
        side = d % 2
        return pltpu.make_async_remote_copy(
            src_ref=send[d].at[slot, side],
            dst_ref=recv[d].at[slot, 1 - side],
            send_sem=ssem.at[slot, d],
            recv_sem=rsem.at[slot, d + 1 - 2 * side],
            device_id=devs[d],
            device_id_type=MESH,
        )

    def incoming(d, slot):
        side = d % 2
        return pltpu.make_async_remote_copy(
            src_ref=send[d].at[slot, side],
            dst_ref=recv[d].at[slot, side],
            send_sem=ssem.at[slot, d],
            recv_sem=rsem.at[slot, d],
            device_id=devs[d],
            device_id_type=MESH,
        )

    def go(d, slot):
        @pl.when(has[d])
        def _():
            outgoing(d, slot).start()

    def start(v, slot):
        x = v.shape[0] // Y
        sx[slot, 0] = v[:Y]
        sx[slot, 1] = v[-Y:]
        go(0, slot)
        go(1, slot)
        for i in range(x):
            sy[slot, 0, i : i + 1] = v[i * Y : i * Y + 1]
            sy[slot, 1, i : i + 1] = v[i * Y + Y - 1 : i * Y + Y]
        go(2, slot)
        go(3, slot)
        for side, lane in ((0, 0), (1, Z - 1)):
            packed = jnp.broadcast_to(v[:Y, lane : lane + 1], (Y, Z))
            for i in range(1, x):
                part = jnp.broadcast_to(v[i * Y : i * Y + Y, lane : lane + 1], (Y, Z))
                packed = jnp.where(lane_y == i, part, packed)
            sz[slot, side] = packed
        go(4, slot)
        go(5, slot)

    def finish(slot):
        for d in range(6):
            @pl.when(has[d])
            def _():
                copy = incoming(d, slot)
                copy.wait_recv()
                copy.wait_send()

    def wide_y(half, x):
        return cat([jnp.broadcast_to(half[i : i + 1], (Y, Z)) for i in range(x)])

    def wide_z(half, x):
        return cat([jnp.broadcast_to(half[:, i : i + 1], (Y, Z)) for i in range(x)])

    def beyond(w, acc, in_x0, in_x1, in_y, in_z):
        x = acc.shape[0] // Y
        acc = acc - w[YB] * in_y - w[ZB] * in_z
        low = w[XM, :Y] * in_x0
        high = w[XP, (x - 1) * Y :] * in_x1
        if x == 1:
            return acc - low - high
        return cat([acc[:Y] - low] + ([acc[Y:-Y]] if x > 2 else []) + [acc[-Y:] - high])

    def operate(v, level, slot):
        w = levs[level]
        x = X >> level
        start(v, slot)
        acc = here.inner(w, v, level)
        finish(slot)
        in_y = jnp.where(rows_of(x) < Y // 2, wide_y(ry[slot, 0], x), wide_y(ry[slot, 1], x))
        in_z = jnp.where(lanes_of(x) < Z // 2, wide_z(rz[slot, 0], x), wide_z(rz[slot, 1], x))
        return beyond(w, acc, rx[slot, 0], rx[slot, 1], in_y, in_z)

    turn = [0]

    def apply(v, level):
        slot = turn[0] % ROUND
        turn[0] += 1
        return operate(v, level, slot)

    def vcycle(r, level, part):
        w = levs[level]
        u = w[INV] * r * (1.0 / MID)
        total = u
        r = r - apply(u, level)
        u = RHO1 * RHO0 * u + 2.0 * RHO1 / HALF * w[INV] * r
        total = total + u
        r = r - apply(u, level)
        coarse = here.restrict(r, level)
        if level + 1 < L:
            e = here.prolong(vcycle(coarse, level + 1, part))
            r = r - apply(e, level)
        else:
            everywhere = collect(coarse, 1, part, gat_pl, gat_x, 4)
            e, ends = spread(world_cycle(everywhere[0], level + 1))
            r = r - beyond(w, here.inner(w, e, level), *ends)
        total = total + e
        u = w[INV] * r * (1.0 / MID)
        total = total + u
        r = r - apply(u, level)
        u = RHO1 * RHO0 * u + 2.0 * RHO1 / HALF * w[INV] * r
        return total + u

    def world_cycle(r, level):
        w = (glev2, glev3)[level - L]

        def apply(v):
            return world.inner(w, v, level - L)

        u = w[INV] * r * (1.0 / MID)
        total = u
        r = r - apply(u)
        u = RHO1 * RHO0 * u + 2.0 * RHO1 / HALF * w[INV] * r
        total = total + u
        r = r - apply(u)
        if level == LEVELS - 1:
            u = RHO2 * RHO1 * u + 2.0 * RHO2 / HALF * w[INV] * r
            return total + u
        e = world.prolong(world_cycle(world.restrict(r, level - L), level + 1))
        total = total + e
        r = r - apply(e)
        u = w[INV] * r * (1.0 / MID)
        total = total + u
        r = r - apply(u)
        u = RHO1 * RHO0 * u + 2.0 * RHO1 / HALF * w[INV] * r
        return total + u

    def hot(shape, wanted):
        at = lax.broadcasted_iota(jnp.int32, shape, 0)
        return jnp.where(at == wanted, 1.0, 0.0)

    def collect(v, fields, part, pl_ref, x_ref, which):
        count = fields * x_own * y_own
        picked[: fields * x_own * Y] = v
        own = picked[pl.ds(0, count, stride=1 << L), :]
        lane = lax.broadcasted_iota(jnp.int32, (Z, GZ), 1) - iz * z_own
        inside = jnp.logical_and(lane >= 0, lane < z_own)
        put = hot((Z, GZ), jnp.where(inside, lane * (1 << L), -1))
        pl_ref[part, my_plane] = dot(own, put)
        gather(pl_ref, part, planes, my_plane, in_plane, which)
        for j in range(ny):
            rows = pl_ref[part, j * nz]
            for k in range(1, nz):
                rows = rows + pl_ref[part, j * nz + k]
            for i in range(fields * x_own):
                x_ref[part, ix, i * GY + j * y_own : i * GY + (j + 1) * y_own] = rows[i * y_own : (i + 1) * y_own]
        gather(x_ref, part, nx, ix, in_column, which + 1)
        return [
            cat([x_ref[part, d, f * x_own * GY : (f + 1) * x_own * GY] for d in range(nx)]) for f in range(fields)
        ]

    def spread(v):
        lane = lax.broadcasted_iota(jnp.int32, (GZ, Z), 1)
        inside = hot((GZ, Z), iz * z_own + lane // (1 << L))
        outside = hot((GZ, Z), jnp.where(lane < Z // 2, iz * z_own - 1, iz * z_own + z_own))
        glob[0, GY : GY + nx * x_own * GY] = dot(v, inside)
        glob[1, GY : GY + nx * x_own * GY] = dot(v, outside)
        rows = rows_of(1)

        def layer(which, a):
            base = (ix * x_own + 1 + a) * GY + iy * y_own
            out = jnp.broadcast_to(glob[which, pl.ds(base, 1), :], (Y, Z))
            for j in range(1, y_own):
                row = jnp.broadcast_to(glob[which, pl.ds(base + j, 1), :], (Y, Z))
                out = jnp.where(rows < j << L, out, row)
            return out

        def rims(a):
            base = (ix * x_own + 1 + a) * GY + iy * y_own
            low = glob[0, pl.ds(base - 1, 1), :] * has_low
            high = glob[0, pl.ds(base + y_own, 1), :] * has_high
            return jnp.where(rows < Y // 2, jnp.broadcast_to(low, (Y, Z)), jnp.broadcast_to(high, (Y, Z)))

        has_low = jnp.where(iy > 0, 1.0, 0.0)
        has_high = jnp.where(iy < ny - 1, 1.0, 0.0)
        own = range(x_own)
        e = here.prolong(cat([layer(0, a) for a in own]))
        in_y = here.prolong(cat([rims(a) for a in own]))
        in_z = here.prolong(cat([layer(1, a) for a in own]))
        return e, (layer(0, -1), layer(0, x_own), in_y, in_z)

    def gather(ref, part, count, me, device, which):
        for j in range(count):
            @pl.when(me != j)
            def _():
                pltpu.make_async_remote_copy(
                    src_ref=ref.at[part, me],
                    dst_ref=ref.at[part, me],
                    send_sem=red_ssem.at[which, part],
                    recv_sem=red_rsem.at[which, part],
                    device_id=device(j),
                    device_id_type=MESH,
                ).start()
        if count > 1:
            others = ref.at[part, pl.ds(0, count - 1)]
            pltpu.make_async_copy(others, others, red_rsem.at[which, part]).wait()
            pltpu.make_async_copy(others, others, red_ssem.at[which, part]).wait()

    def in_plane(j):
        return (ix, j // nz, j % nz)

    def in_column(j):
        return (j, iy, iz)

    my_plane = iy * nz + iz

    def reduce_plane(ref, part, value, which):
        ref[part, my_plane] = value
        gather(ref, part, planes, my_plane, in_plane, which)
        return jnp.sum(ref[part], axis=0)

    def reduce_column(ref, part, value, which):
        ref[part, ix] = value
        gather(ref, part, nx, ix, in_column, which)
        return jnp.sum(ref[part], axis=0)

    def total_of(v):
        return jnp.sum(jnp.sum(v, axis=0, keepdims=True), axis=1, keepdims=True)

    def lane_of(row, i):
        return jnp.sum(jnp.where(lane_1 == i, row, 0.0), axis=1, keepdims=True)

    it = it_ref[...].reshape(X * Y, Z)
    reaction = rea_ref[...].reshape(X * Y, Z)
    start(it, KEPT)
    finish(KEPT)
    rows, lanes = rows_of(X), lanes_of(X)
    last_row, last_lane = rows == Y - 1, lanes == Z - 1
    n_xm = cat([rx[KEPT, 0], it[:-Y]])
    n_xp = cat([it[Y:], rx[KEPT, 1]])
    n_ym = jnp.where(rows == 0, wide_y(ry[KEPT, 0], X), roll(it, 1, 0))
    n_yp = jnp.where(last_row, wide_y(ry[KEPT, 1], X), roll(it, -1, 0))
    n_zm = jnp.where(lanes == 0, wide_z(rz[KEPT, 0], X), roll(it, 1, 1))
    n_zp = jnp.where(last_lane, wide_z(rz[KEPT, 1], X), roll(it, -1, 1))
    ws = []
    r = src_ref[...].reshape(X * Y, Z) - reaction * it
    for sign, n in ((-1, n_xm), (1, n_xp), (-1, n_ym), (1, n_yp), (-1, n_zm), (1, n_zp)):
        g = n - it
        square = g * g
        root = jnp.sqrt(1.0 + square)
        ws.append((1.0 + 2.0 * square) / root)
        r = r + g * root
    rem_ref[...] = r.reshape(X, Y, Z)
    here.put(levs[0], 0, ws, reaction)
    for level in range(L):
        ws, reaction = here.coarsen(ws, reaction, level)
        if level + 1 < L:
            here.put(levs[level + 1], level + 1, ws, reaction)
    glob[...] = jnp.zeros_like(glob)
    *ws, reaction = collect(cat(list(ws) + [reaction]), 7, 0, set_pl, set_x, 6)
    world.put(glev2, 0, ws, reaction)
    world.put(glev3, 1, *world.coarsen(ws, reaction, 0))
    for ref in (p_ref, q_ref, phx, phy, phz, dhx, dhy, dhz):
        ref[...] = jnp.zeros_like(ref)
    dir_ref[...] = jnp.zeros_like(dir_ref)

    def body(it_idx, carry):
        rz_old, pq_old = carry
        part = lax.rem(it_idx, 2)
        r = rem_ref[...].reshape(X * Y, Z)
        turn[0] = 0
        z = vcycle(r, 0, part)
        z_slot = turn[0] % ROUND
        az = apply(z, 0)
        q_old = q_ref[...]
        sums = jnp.where(
            lane_1 == 0,
            total_of(rem_ref[...].reshape(X * Y, Z) * z),
            jnp.where(lane_1 == 1, total_of(z * az), total_of(z * q_old)),
        )
        row = reduce_plane(dot_pl, part, sums, 0)
        row = reduce_column(dot_x, part, row, 1)
        rz_new, zaz, zq = lane_of(row, 0), lane_of(row, 1), lane_of(row, 2)
        beta = rz_new / rz_old
        pq = zaz + 2.0 * beta * zq + beta * beta * pq_old
        a = rz_new / pq
        p = z + beta * p_ref[...]
        q = az + beta * q_old
        p_ref[...] = p
        q_ref[...] = q
        dir_ref[...] = dir_ref[...] + (a * p).reshape(X, Y, Z)
        rem_ref[...] = rem_ref[...] - (a * q).reshape(X, Y, Z)
        for got, ph, dh in ((rx, phx, dhx), (ry, phy, dhy), (rz, phz, dhz)):
            for side in range(2):
                edge = got[z_slot, side] + beta * ph[side]
                ph[side] = edge
                dh[side] = dh[side] + a * edge
        return rz_new, pq

    one = jnp.ones((1, 1), jnp.float32)
    lax.fori_loop(0, ITERS, body, (one, jnp.zeros((1, 1), jnp.float32)))

    it = it_ref[...].reshape(X * Y, Z)
    step_dir = dir_ref[...].reshape(X * Y, Z)

    def energy(g):
        square = 1.0 + g * g
        return (square * jnp.sqrt(square) - 1.0) * (1.0 / 3.0)

    ends_y = jnp.where(jnp.logical_and(last_row, iy == ny - 1), 1.0, 0.0)
    ends_z = jnp.where(jnp.logical_and(last_lane, iz == nz - 1), 1.0, 0.0)
    ends_x = jnp.where(ix == nx - 1, 1.0, 0.0)
    across = lax.broadcasted_iota(jnp.int32, (X, Z), 0) == lax.broadcasted_iota(jnp.int32, (X, Z), 1)
    trial_rows = []
    for k in range(TRIALS):
        s = jnp.exp2(-jnp.full((1, Z), tp_ref[k], jnp.int32).astype(jnp.float32))
        v = it + s * step_dir
        low_x = cat([rx[KEPT, 0] + s * dhx[0], v[:-Y]])
        low_y = jnp.where(rows == 0, wide_y(ry[KEPT, 0] + s * dhy[0], X), roll(v, 1, 0))
        low_z = jnp.where(lanes == 0, wide_z(rz[KEPT, 0] + s * dhz[0], X), roll(v, 1, 1))
        at_end = energy(v)
        e = energy(v - low_x) + energy(v - low_y) + energy(v - low_z)
        e = e + at_end * (ends_y + ends_z)
        e = cat([e[:-Y], e[-Y:] + ends_x * at_end[-Y:]]) if X > 1 else e + ends_x * at_end
        e = e + 0.5 * rea_ref[...].reshape(X * Y, Z) * v * v - src_ref[...].reshape(X * Y, Z) * v
        by_layer = jnp.sum(jnp.sum(e.reshape(X, Y, Z), axis=1), axis=1, keepdims=True)
        trial_rows.append(jnp.sum(jnp.where(across, by_layer, 0.0), axis=0, keepdims=True))
    layers = reduce_plane(en_pl, 0, jnp.concatenate(trial_rows, axis=0), 2)
    layers = layers / (Y * ny * Z * nz)
    le_ref[...] = layers[:, :X]
    overall = reduce_column(en_x, 0, layers, 3)
    overall = jnp.sum(overall, axis=1, keepdims=True) / (X * nx)
    en_ref[...] = jnp.broadcast_to(overall, (TRIALS, Z))


def on_device(counts, iterate, source, reaction, trial_powers):
    X, Y, Z = iterate.shape
    nx, ny, nz = counts
    f32 = jnp.float32
    slots = ROUND + 1
    vm = pltpu.VMEM
    scratch = [vm((slots, 2, rows, Z), f32) for rows in (Y, Y, X, X, Y, Y)]
    scratch += [pltpu.SemaphoreType.DMA((slots, 6))] * 2
    x_own, y_own = X // 4, Y // 4
    GX, GY, GZ = nx * x_own, ny * y_own, nz * Z // 4
    scratch += [vm((10, (X >> level) * Y, Z), f32) for level in range(2)]
    scratch += [vm((8, (GX >> level) * GY, GZ), f32) for level in range(2)]
    scratch += [vm((X * Y, Z), f32)] * 2
    scratch += [vm((2, rows, Z), f32) for rows in (Y, X, Y)] * 2
    scratch += [
        vm((2, ny * nz, 1, Z), f32), vm((2, nx, 1, Z), f32),
        vm((1, ny * nz, TRIALS, Z), f32), vm((1, nx, TRIALS, Z), f32),
        pltpu.SemaphoreType.DMA((8, 2)), pltpu.SemaphoreType.DMA((8, 2)),
        vm((7 * x_own * Y, Z), f32),
        vm((2, ny * nz, x_own * y_own, GZ), f32), vm((2, nx, x_own * GY, GZ), f32),
        vm((1, ny * nz, 7 * x_own * y_own, GZ), f32), vm((1, nx, 7 * x_own * GY, GZ), f32),
        vm((2, (GX + 2) * GY, Z), f32),
    ]
    whole = pl.BlockSpec(memory_space=pltpu.VMEM)
    out = pl.pallas_call(
        functools.partial(kernel, (X, Y, Z), counts),
        out_shape=[
            jax.ShapeDtypeStruct((X, Y, Z), f32),
            jax.ShapeDtypeStruct((X, Y, Z), f32),
            jax.ShapeDtypeStruct((TRIALS, X), f32),
            jax.ShapeDtypeStruct((TRIALS, Z), f32),
        ],
        in_specs=[pl.BlockSpec(memory_space=pltpu.SMEM), whole, whole, whole],
        out_specs=[whole] * 4,
        scratch_shapes=scratch,
        compiler_params=pltpu.CompilerParams(has_side_effects=True, vmem_limit_bytes=48 * 1024 * 1024),
        name="newton_step",
    )(trial_powers, iterate, source, reaction)
    return out[0], out[1], out[2], out[3][:, 0]


def solution(mesh):
    counts = tuple(mesh.shape[axis] for axis in ("gx", "gy", "gz"))
    grid = P("gx", "gy", "gz")
    return jax.shard_map(
        functools.partial(on_device, counts),
        mesh=mesh,
        in_specs=(grid, grid, grid, P()),
        out_specs=(grid, grid, P(None, "gx"), P()),
        check_vma=False,
    )
```

```python
import functools

import jax
import jax.numpy as jnp
from jax import lax
from jax.experimental import pallas as pl
from jax.experimental.pallas import tpu as pltpu
from jax.sharding import PartitionSpec as P

ITERS = 4
LEVELS = 4
TRIALS = 4
MID = 1.15
HALF = 0.85
SIGMA = MID / HALF
RHO0 = 1.0 / SIGMA
RHO1 = 1.0 / (2.0 * SIGMA - RHO0)
RHO2 = 1.0 / (2.0 * SIGMA - RHO1)
ROUND = 3
KEPT = ROUND
DG, INV, XM, XP, YM, YP, ZM, ZP, YB, ZB = range(10)
MESH = pl.DeviceIdType.MESH


class Grid:
    def __init__(self, Y, Z):
        self.Y, self.Z = Y, Z

    def rows_of(self, x):
        return lax.rem(lax.broadcasted_iota(jnp.int32, (x * self.Y, self.Z), 0), self.Y)

    def lanes_of(self, x):
        return lax.broadcasted_iota(jnp.int32, (x * self.Y, self.Z), 1)

    def pair_x(self, v):
        Y = self.Y
        x = v.shape[0] // Y
        return cat([v[2 * i * Y : (2 * i + 1) * Y] + v[(2 * i + 1) * Y : (2 * i + 2) * Y] for i in range(x // 2)])

    def pick_x(self, v, odd):
        Y = self.Y
        x = v.shape[0] // Y
        return cat([v[(2 * i + odd) * Y : (2 * i + odd + 1) * Y] for i in range(x // 2)])

    def bit(self, v, level, axis):
        at = self.rows_of(v.shape[0] // self.Y) if axis == 0 else self.lanes_of(v.shape[0] // self.Y)
        return lax.rem(at, 2 << level) < (1 << level)

    def pair(self, v, level, axis):
        step = 1 << level
        return v + jnp.where(self.bit(v, level, axis), roll(v, -step, axis), roll(v, step, axis))

    def pick(self, v, level, axis, odd):
        step = 1 << level
        low = self.bit(v, level, axis)
        if odd:
            return jnp.where(low, roll(v, -step, axis), v)
        return jnp.where(low, v, roll(v, step, axis))

    def restrict(self, v, level):
        return self.pair(self.pair(self.pair_x(v), level, 0), level, 1)

    def prolong(self, v):
        Y = self.Y
        x = v.shape[0] // Y
        return cat([v[(i // 2) * Y : (i // 2 + 1) * Y] for i in range(2 * x)])

    def coarsen(self, ws, reaction, level):
        xm, xp, ym, yp, zm, zp = ws
        pair, pick = self.pair, self.pick
        ws = (
            pair(pair(self.pick_x(xm, 0), level, 0), level, 1),
            pair(pair(self.pick_x(xp, 1), level, 0), level, 1),
            pair(pick(self.pair_x(ym), level, 0, 0), level, 1),
            pair(pick(self.pair_x(yp), level, 0, 1), level, 1),
            pick(pair(self.pair_x(zm), level, 0), level, 1, 0),
            pick(pair(self.pair_x(zp), level, 0), level, 1, 1),
        )
        return ws, self.restrict(reaction, level)

    def put(self, w, level, ws, reaction):
        Y, Z = self.Y, self.Z
        xm, xp, ym, yp, zm, zp = ws
        step = 1 << level
        x = xm.shape[0] // Y
        rows, lanes = self.rows_of(x), self.lanes_of(x)
        diagonal = reaction + xm + xp + ym + yp + zm + zp
        zero = jnp.zeros_like(xm)
        w[DG] = diagonal
        w[INV] = 1.0 / diagonal
        w[XM] = xm
        w[XP] = xp
        w[YM] = jnp.where(rows < step, zero, ym)
        w[YP] = jnp.where(rows >= Y - step, zero, yp)
        w[ZM] = jnp.where(lanes < step, zero, zm)
        w[ZP] = jnp.where(lanes >= Z - step, zero, zp)
        if w.shape[0] > YB:
            w[YB] = jnp.where(rows < step, ym, jnp.where(rows >= Y - step, yp, zero))
            w[ZB] = jnp.where(lanes < step, zm, jnp.where(lanes >= Z - step, zp, zero))

    def inner(self, w, v, level):
        step = 1 << level
        acc = w[DG] * v
        acc = acc - w[YM] * roll(v, step, 0) - w[YP] * roll(v, -step, 0)
        acc = acc - w[ZM] * roll(v, step, 1) - w[ZP] * roll(v, -step, 1)
        Y = self.Y
        if v.shape[0] > Y:
            none = jnp.zeros((Y, self.Z), jnp.float32)
            acc = acc - w[XM] * cat([none, v[:-Y]]) - w[XP] * cat([v[Y:], none])
        return acc


def cat(parts):
    return parts[0] if len(parts) == 1 else jnp.concatenate(parts, axis=0)


def roll(v, shift, axis):
    return pltpu.roll(v, shift % v.shape[axis], axis)


def dot(a, b):
    return lax.dot_general(
        a, b, (((1,), (0,)), ((), ())), precision=lax.Precision.HIGHEST, preferred_element_type=jnp.float32
    )


def kernel(
    sizes, counts, tp_ref, it_ref, src_ref, rea_ref, dir_ref, rem_ref, le_ref, en_ref,
    sx, rx, sy, ry, sz, rz, ssem, rsem, lev0, lev1, glev2, glev3, p_ref, q_ref,
    phx, phy, phz, dhx, dhy, dhz, dot_all, en_pl, en_x, red_ssem, red_rsem,
    picked, gat_pl, gat_x, set_pl, set_x, glob,
):
    X, Y, Z = sizes
    nx, ny, nz = counts
    planes = ny * nz
    levs = (lev0, lev1)
    L = len(levs)
    x_own, y_own, z_own = X >> L, Y >> L, Z >> L
    GY, GZ = ny * y_own, nz * z_own
    here, world = Grid(Y, Z), Grid(GY, GZ)
    rows_of, lanes_of = here.rows_of, here.lanes_of
    ix, iy, iz = lax.axis_index("gx"), lax.axis_index("gy"), lax.axis_index("gz")
    has = (ix > 0, ix < nx - 1, iy > 0, iy < ny - 1, iz > 0, iz < nz - 1)
    devs = (
        (ix - 1, iy, iz), (ix + 1, iy, iz), (ix, iy - 1, iz),
        (ix, iy + 1, iz), (ix, iy, iz - 1), (ix, iy, iz + 1),
    )
    send = (sx, sx, sy, sy, sz, sz)
    recv = (rx, rx, ry, ry, rz, rz)
    lane_y = lax.broadcasted_iota(jnp.int32, (Y, Z), 1)
    lane_1 = lax.broadcasted_iota(jnp.int32, (1, Z), 1)

    for d in range(6):
        @pl.when(jnp.logical_not(has[d]))
        def _():
            recv[d][:, d % 2] = jnp.zeros(recv[d].shape[:1] + recv[d].shape[2:], jnp.float32)

    def outgoing(d, slot):
        side = d % 2
        return pltpu.make_async_remote_copy(
            src_ref=send[d].at[slot, side],
            dst_ref=recv[d].at[slot, 1 - side],
            send_sem=ssem.at[slot, d],
            recv_sem=rsem.at[slot, d + 1 - 2 * side],
            device_id=devs[d],
            device_id_type=MESH,
        )

    def incoming(d, slot):
        side = d % 2
        return pltpu.make_async_remote_copy(
            src_ref=send[d].at[slot, side],
            dst_ref=recv[d].at[slot, side],
            send_sem=ssem.at[slot, d],
            recv_sem=rsem.at[slot, d],
            device_id=devs[d],
            device_id_type=MESH,
        )

    def go(d, slot):
        @pl.when(has[d])
        def _():
            outgoing(d, slot).start()

    def start(v, slot):
        x = v.shape[0] // Y
        sx[slot, 0] = v[:Y]
        sx[slot, 1] = v[-Y:]
        go(0, slot)
        go(1, slot)
        for i in range(x):
            sy[slot, 0, i : i + 1] = v[i * Y : i * Y + 1]
            sy[slot, 1, i : i + 1] = v[i * Y + Y - 1 : i * Y + Y]
        go(2, slot)
        go(3, slot)
        for side, lane in ((0, 0), (1, Z - 1)):
            packed = jnp.broadcast_to(v[:Y, lane : lane + 1], (Y, Z))
            for i in range(1, x):
                part = jnp.broadcast_to(v[i * Y : i * Y + Y, lane : lane + 1], (Y, Z))
                packed = jnp.where(lane_y == i, part, packed)
            sz[slot, side] = packed
        go(4, slot)
        go(5, slot)

    def finish(slot):
        for d in range(6):
            @pl.when(has[d])
            def _():
                copy = incoming(d, slot)
                copy.wait_recv()
                copy.wait_send()

    def wide_y(half, x):
        return cat([jnp.broadcast_to(half[i : i + 1], (Y, Z)) for i in range(x)])

    def wide_z(half, x):
        return cat([jnp.broadcast_to(half[:, i : i + 1], (Y, Z)) for i in range(x)])

    def beyond(w, acc, in_x0, in_x1, in_y, in_z):
        x = acc.shape[0] // Y
        acc = acc - w[YB] * in_y - w[ZB] * in_z
        low = w[XM, :Y] * in_x0
        high = w[XP, (x - 1) * Y :] * in_x1
        if x == 1:
            return acc - low - high
        return cat([acc[:Y] - low] + ([acc[Y:-Y]] if x > 2 else []) + [acc[-Y:] - high])

    def operate(v, level, slot):
        w = levs[level]
        x = X >> level
        start(v, slot)
        acc = here.inner(w, v, level)
        finish(slot)
        in_y = jnp.where(rows_of(x) < Y // 2, wide_y(ry[slot, 0], x), wide_y(ry[slot, 1], x))
        in_z = jnp.where(lanes_of(x) < Z // 2, wide_z(rz[slot, 0], x), wide_z(rz[slot, 1], x))
        return beyond(w, acc, rx[slot, 0], rx[slot, 1], in_y, in_z)

    turn = [0]

    def apply(v, level):
        slot = turn[0] % ROUND
        turn[0] += 1
        return operate(v, level, slot)

    def vcycle(r, level, part):
        w = levs[level]
        u = w[INV] * r * (1.0 / MID)
        total = u
        r = r - apply(u, level)
        u = RHO1 * RHO0 * u + 2.0 * RHO1 / HALF * w[INV] * r
        total = total + u
        r = r - apply(u, level)
        coarse = here.restrict(r, level)
        if level + 1 < L:
            e = here.prolong(vcycle(coarse, level + 1, part))
            r = r - apply(e, level)
        else:
            everywhere = collect(coarse, 1, part, gat_pl, gat_x, 4)
            e, ends = spread(world_cycle(everywhere[0], level + 1))
            r = r - beyond(w, here.inner(w, e, level), *ends)
        total = total + e
        u = w[INV] * r * (1.0 / MID)
        total = total + u
        r = r - apply(u, level)
        u = RHO1 * RHO0 * u + 2.0 * RHO1 / HALF * w[INV] * r
        return total + u

    def world_cycle(r, level):
        w = (glev2, glev3)[level - L]

        def apply(v):
            return world.inner(w, v, level - L)

        u = w[INV] * r * (1.0 / MID)
        total = u
        r = r - apply(u)
        u = RHO1 * RHO0 * u + 2.0 * RHO1 / HALF * w[INV] * r
        total = total + u
        r = r - apply(u)
        if level == LEVELS - 1:
            u = RHO2 * RHO1 * u + 2.0 * RHO2 / HALF * w[INV] * r
            return total + u
        e = world.prolong(world_cycle(world.restrict(r, level - L), level + 1))
        total = total + e
        r = r - apply(e)
        u = w[INV] * r * (1.0 / MID)
        total = total + u
        r = r - apply(u)
        u = RHO1 * RHO0 * u + 2.0 * RHO1 / HALF * w[INV] * r
        return total + u

    def hot(shape, wanted):
        at = lax.broadcasted_iota(jnp.int32, shape, 0)
        return jnp.where(at == wanted, 1.0, 0.0)

    def collect(v, fields, part, pl_ref, x_ref, which):
        count = fields * x_own * y_own
        picked[: fields * x_own * Y] = v
        own = picked[pl.ds(0, count, stride=1 << L), :]
        lane = lax.broadcasted_iota(jnp.int32, (Z, GZ), 1) - iz * z_own
        inside = jnp.logical_and(lane >= 0, lane < z_own)
        put = hot((Z, GZ), jnp.where(inside, lane * (1 << L), -1))
        pl_ref[part, my_plane] = dot(own, put)
        gather(pl_ref, part, planes, my_plane, in_plane, which)
        for j in range(ny):
            rows = pl_ref[part, j * nz]
            for k in range(1, nz):
                rows = rows + pl_ref[part, j * nz + k]
            for i in range(fields * x_own):
                x_ref[part, ix, i * GY + j * y_own : i * GY + (j + 1) * y_own] = rows[i * y_own : (i + 1) * y_own]
        gather(x_ref, part, nx, ix, in_column, which + 1)
        return [
            cat([x_ref[part, d, f * x_own * GY : (f + 1) * x_own * GY] for d in range(nx)]) for f in range(fields)
        ]

    def spread(v):
        lane = lax.broadcasted_iota(jnp.int32, (GZ, Z), 1)
        inside = hot((GZ, Z), iz * z_own + lane // (1 << L))
        outside = hot((GZ, Z), jnp.where(lane < Z // 2, iz * z_own - 1, iz * z_own + z_own))
        glob[0, GY : GY + nx * x_own * GY] = dot(v, inside)
        glob[1, GY : GY + nx * x_own * GY] = dot(v, outside)
        rows = rows_of(1)

        def layer(which, a):
            base = (ix * x_own + 1 + a) * GY + iy * y_own
            out = jnp.broadcast_to(glob[which, pl.ds(base, 1), :], (Y, Z))
            for j in range(1, y_own):
                row = jnp.broadcast_to(glob[which, pl.ds(base + j, 1), :], (Y, Z))
                out = jnp.where(rows < j << L, out, row)
            return out

        def rims(a):
            base = (ix * x_own + 1 + a) * GY + iy * y_own
            low = glob[0, pl.ds(base - 1, 1), :] * has_low
            high = glob[0, pl.ds(base + y_own, 1), :] * has_high
            return jnp.where(rows < Y // 2, jnp.broadcast_to(low, (Y, Z)), jnp.broadcast_to(high, (Y, Z)))

        has_low = jnp.where(iy > 0, 1.0, 0.0)
        has_high = jnp.where(iy < ny - 1, 1.0, 0.0)
        own = range(x_own)
        e = here.prolong(cat([layer(0, a) for a in own]))
        in_y = here.prolong(cat([rims(a) for a in own]))
        in_z = here.prolong(cat([layer(1, a) for a in own]))
        return e, (layer(0, -1), layer(0, x_own), in_y, in_z)

    def gather(ref, part, count, me, device, which):
        for j in range(count):
            @pl.when(me != j)
            def _():
                pltpu.make_async_remote_copy(
                    src_ref=ref.at[part, me],
                    dst_ref=ref.at[part, me],
                    send_sem=red_ssem.at[which, part],
                    recv_sem=red_rsem.at[which, part],
                    device_id=device(j),
                    device_id_type=MESH,
                ).start()
        if count > 1:
            others = ref.at[part, pl.ds(0, count - 1)]
            pltpu.make_async_copy(others, others, red_rsem.at[which, part]).wait()
            pltpu.make_async_copy(others, others, red_ssem.at[which, part]).wait()

    def in_plane(j):
        return (ix, j // nz, j % nz)

    def in_column(j):
        return (j, iy, iz)

    def in_grid(j):
        return (j // planes, j // nz % ny, j % nz)

    my_plane = iy * nz + iz
    me = ix * planes + my_plane

    def reduce_plane(ref, part, value, which):
        ref[part, my_plane] = value
        gather(ref, part, planes, my_plane, in_plane, which)
        return jnp.sum(ref[part], axis=0)

    def reduce_column(ref, part, value, which):
        ref[part, ix] = value
        gather(ref, part, nx, ix, in_column, which)
        return jnp.sum(ref[part], axis=0)

    def total_of(v):
        return jnp.sum(jnp.sum(v, axis=0, keepdims=True), axis=1, keepdims=True)

    def lane_of(row, i):
        return jnp.sum(jnp.where(lane_1 == i, row, 0.0), axis=1, keepdims=True)

    it = it_ref[...].reshape(X * Y, Z)
    reaction = rea_ref[...].reshape(X * Y, Z)
    start(it, KEPT)
    finish(KEPT)
    rows, lanes = rows_of(X), lanes_of(X)
    last_row, last_lane = rows == Y - 1, lanes == Z - 1
    n_xm = cat([rx[KEPT, 0], it[:-Y]])
    n_xp = cat([it[Y:], rx[KEPT, 1]])
    n_ym = jnp.where(rows == 0, wide_y(ry[KEPT, 0], X), roll(it, 1, 0))
    n_yp = jnp.where(last_row, wide_y(ry[KEPT, 1], X), roll(it, -1, 0))
    n_zm = jnp.where(lanes == 0, wide_z(rz[KEPT, 0], X), roll(it, 1, 1))
    n_zp = jnp.where(last_lane, wide_z(rz[KEPT, 1], X), roll(it, -1, 1))
    ws = []
    r = src_ref[...].reshape(X * Y, Z) - reaction * it
    for sign, n in ((-1, n_xm), (1, n_xp), (-1, n_ym), (1, n_yp), (-1, n_zm), (1, n_zp)):
        g = n - it
        square = g * g
        root = jnp.sqrt(1.0 + square)
        ws.append((1.0 + 2.0 * square) / root)
        r = r + g * root
    rem_ref[...] = r.reshape(X, Y, Z)
    here.put(levs[0], 0, ws, reaction)
    for level in range(L):
        ws, reaction = here.coarsen(ws, reaction, level)
        if level + 1 < L:
            here.put(levs[level + 1], level + 1, ws, reaction)
    glob[...] = jnp.zeros_like(glob)
    *ws, reaction = collect(cat(list(ws) + [reaction]), 7, 0, set_pl, set_x, 6)
    world.put(glev2, 0, ws, reaction)
    world.put(glev3, 1, *world.coarsen(ws, reaction, 0))
    for ref in (p_ref, q_ref, phx, phy, phz, dhx, dhy, dhz):
        ref[...] = jnp.zeros_like(ref)
    dir_ref[...] = jnp.zeros_like(dir_ref)

    def body(it_idx, carry):
        rz_old, pq_old = carry
        part = lax.rem(it_idx, 2)
        r = rem_ref[...].reshape(X * Y, Z)
        turn[0] = 0
        z = vcycle(r, 0, part)
        z_slot = turn[0] % ROUND
        az = apply(z, 0)
        q_old = q_ref[...]
        sums = jnp.where(
            lane_1 == 0,
            total_of(rem_ref[...].reshape(X * Y, Z) * z),
            jnp.where(lane_1 == 1, total_of(z * az), total_of(z * q_old)),
        )
        dot_all[part, me] = sums
        gather(dot_all, part, nx * planes, me, in_grid, 0)
        row = jnp.sum(dot_all[part], axis=0)
        rz_new, zaz, zq = lane_of(row, 0), lane_of(row, 1), lane_of(row, 2)
        beta = rz_new / rz_old
        pq = zaz + 2.0 * beta * zq + beta * beta * pq_old
        a = rz_new / pq
        p = z + beta * p_ref[...]
        q = az + beta * q_old
        p_ref[...] = p
        q_ref[...] = q
        dir_ref[...] = dir_ref[...] + (a * p).reshape(X, Y, Z)
        rem_ref[...] = rem_ref[...] - (a * q).reshape(X, Y, Z)
        for got, ph, dh in ((rx, phx, dhx), (ry, phy, dhy), (rz, phz, dhz)):
            for side in range(2):
                edge = got[z_slot, side] + beta * ph[side]
                ph[side] = edge
                dh[side] = dh[side] + a * edge
        return rz_new, pq

    one = jnp.ones((1, 1), jnp.float32)
    lax.fori_loop(0, ITERS, body, (one, jnp.zeros((1, 1), jnp.float32)))

    it = it_ref[...].reshape(X * Y, Z)
    step_dir = dir_ref[...].reshape(X * Y, Z)

    def energy(g):
        square = 1.0 + g * g
        return (square * jnp.sqrt(square) - 1.0) * (1.0 / 3.0)

    ends_y = jnp.where(jnp.logical_and(last_row, iy == ny - 1), 1.0, 0.0)
    ends_z = jnp.where(jnp.logical_and(last_lane, iz == nz - 1), 1.0, 0.0)
    ends_x = jnp.where(ix == nx - 1, 1.0, 0.0)
    across = lax.broadcasted_iota(jnp.int32, (X, Z), 0) == lax.broadcasted_iota(jnp.int32, (X, Z), 1)
    trial_rows = []
    for k in range(TRIALS):
        s = jnp.exp2(-jnp.full((1, Z), tp_ref[k], jnp.int32).astype(jnp.float32))
        v = it + s * step_dir
        low_x = cat([rx[KEPT, 0] + s * dhx[0], v[:-Y]])
        low_y = jnp.where(rows == 0, wide_y(ry[KEPT, 0] + s * dhy[0], X), roll(v, 1, 0))
        low_z = jnp.where(lanes == 0, wide_z(rz[KEPT, 0] + s * dhz[0], X), roll(v, 1, 1))
        at_end = energy(v)
        e = energy(v - low_x) + energy(v - low_y) + energy(v - low_z)
        e = e + at_end * (ends_y + ends_z)
        e = cat([e[:-Y], e[-Y:] + ends_x * at_end[-Y:]]) if X > 1 else e + ends_x * at_end
        e = e + 0.5 * rea_ref[...].reshape(X * Y, Z) * v * v - src_ref[...].reshape(X * Y, Z) * v
        by_layer = jnp.sum(jnp.sum(e.reshape(X, Y, Z), axis=1), axis=1, keepdims=True)
        trial_rows.append(jnp.sum(jnp.where(across, by_layer, 0.0), axis=0, keepdims=True))
    layers = reduce_plane(en_pl, 0, jnp.concatenate(trial_rows, axis=0), 2)
    layers = layers / (Y * ny * Z * nz)
    le_ref[...] = layers[:, :X]
    overall = reduce_column(en_x, 0, layers, 3)
    overall = jnp.sum(overall, axis=1, keepdims=True) / (X * nx)
    en_ref[...] = jnp.broadcast_to(overall, (TRIALS, Z))


def on_device(counts, iterate, source, reaction, trial_powers):
    X, Y, Z = iterate.shape
    nx, ny, nz = counts
    f32 = jnp.float32
    slots = ROUND + 1
    vm = pltpu.VMEM
    scratch = [vm((slots, 2, rows, Z), f32) for rows in (Y, Y, X, X, Y, Y)]
    scratch += [pltpu.SemaphoreType.DMA((slots, 6))] * 2
    x_own, y_own = X // 4, Y // 4
    GX, GY, GZ = nx * x_own, ny * y_own, nz * Z // 4
    scratch += [vm((10, (X >> level) * Y, Z), f32) for level in range(2)]
    scratch += [vm((8, (GX >> level) * GY, GZ), f32) for level in range(2)]
    scratch += [vm((X * Y, Z), f32)] * 2
    scratch += [vm((2, rows, Z), f32) for rows in (Y, X, Y)] * 2
    scratch += [
        vm((2, nx * ny * nz, 1, Z), f32),
        vm((1, ny * nz, TRIALS, Z), f32), vm((1, nx, TRIALS, Z), f32),
        pltpu.SemaphoreType.DMA((8, 2)), pltpu.SemaphoreType.DMA((8, 2)),
        vm((7 * x_own * Y, Z), f32),
        vm((2, ny * nz, x_own * y_own, GZ), f32), vm((2, nx, x_own * GY, GZ), f32),
        vm((1, ny * nz, 7 * x_own * y_own, GZ), f32), vm((1, nx, 7 * x_own * GY, GZ), f32),
        vm((2, (GX + 2) * GY, Z), f32),
    ]
    whole = pl.BlockSpec(memory_space=pltpu.VMEM)
    out = pl.pallas_call(
        functools.partial(kernel, (X, Y, Z), counts),
        out_shape=[
            jax.ShapeDtypeStruct((X, Y, Z), f32),
            jax.ShapeDtypeStruct((X, Y, Z), f32),
            jax.ShapeDtypeStruct((TRIALS, X), f32),
            jax.ShapeDtypeStruct((TRIALS, Z), f32),
        ],
        in_specs=[pl.BlockSpec(memory_space=pltpu.SMEM), whole, whole, whole],
        out_specs=[whole] * 4,
        scratch_shapes=scratch,
        compiler_params=pltpu.CompilerParams(has_side_effects=True, vmem_limit_bytes=48 * 1024 * 1024),
        name="newton_step",
    )(trial_powers, iterate, source, reaction)
    return out[0], out[1], out[2], out[3][:, 0]


def solution(mesh):
    counts = tuple(mesh.shape[axis] for axis in ("gx", "gy", "gz"))
    grid = P("gx", "gy", "gz")
    return jax.shard_map(
        functools.partial(on_device, counts),
        mesh=mesh,
        in_specs=(grid, grid, grid, P()),
        out_specs=(grid, grid, P(None, "gx"), P()),
        check_vma=False,
    )
```

```python
import functools

import jax
import jax.numpy as jnp
from jax import lax
from jax.experimental import pallas as pl
from jax.experimental.pallas import tpu as pltpu
from jax.sharding import PartitionSpec as P

ITERS = 4
LEVELS = 4
TRIALS = 4
MID = 1.15
HALF = 0.85
SIGMA = MID / HALF
RHO0 = 1.0 / SIGMA
RHO1 = 1.0 / (2.0 * SIGMA - RHO0)
RHO2 = 1.0 / (2.0 * SIGMA - RHO1)
ROUND = 3
KEPT = ROUND
DG, INV, XM, XP, YM, YP, ZM, ZP, YB, ZB = range(10)
MESH = pl.DeviceIdType.MESH


class Grid:
    def __init__(self, Y, Z):
        self.Y, self.Z = Y, Z

    def rows_of(self, x):
        return lax.rem(lax.broadcasted_iota(jnp.int32, (x * self.Y, self.Z), 0), self.Y)

    def lanes_of(self, x):
        return lax.broadcasted_iota(jnp.int32, (x * self.Y, self.Z), 1)

    def pair_x(self, v):
        Y = self.Y
        x = v.shape[0] // Y
        return cat([v[2 * i * Y : (2 * i + 1) * Y] + v[(2 * i + 1) * Y : (2 * i + 2) * Y] for i in range(x // 2)])

    def pick_x(self, v, odd):
        Y = self.Y
        x = v.shape[0] // Y
        return cat([v[(2 * i + odd) * Y : (2 * i + odd + 1) * Y] for i in range(x // 2)])

    def bit(self, v, level, axis):
        at = self.rows_of(v.shape[0] // self.Y) if axis == 0 else self.lanes_of(v.shape[0] // self.Y)
        return lax.rem(at, 2 << level) < (1 << level)

    def pair(self, v, level, axis):
        step = 1 << level
        return v + jnp.where(self.bit(v, level, axis), roll(v, -step, axis), roll(v, step, axis))

    def pick(self, v, level, axis, odd):
        step = 1 << level
        low = self.bit(v, level, axis)
        if odd:
            return jnp.where(low, roll(v, -step, axis), v)
        return jnp.where(low, v, roll(v, step, axis))

    def restrict(self, v, level):
        return self.pair(self.pair(self.pair_x(v), level, 0), level, 1)

    def prolong(self, v):
        Y = self.Y
        x = v.shape[0] // Y
        return cat([v[(i // 2) * Y : (i // 2 + 1) * Y] for i in range(2 * x)])

    def coarsen(self, ws, reaction, level):
        xm, xp, ym, yp, zm, zp = ws
        pair, pick = self.pair, self.pick
        ws = (
            pair(pair(self.pick_x(xm, 0), level, 0), level, 1),
            pair(pair(self.pick_x(xp, 1), level, 0), level, 1),
            pair(pick(self.pair_x(ym), level, 0, 0), level, 1),
            pair(pick(self.pair_x(yp), level, 0, 1), level, 1),
            pick(pair(self.pair_x(zm), level, 0), level, 1, 0),
            pick(pair(self.pair_x(zp), level, 0), level, 1, 1),
        )
        return ws, self.restrict(reaction, level)

    def put(self, w, level, ws, reaction):
        Y, Z = self.Y, self.Z
        xm, xp, ym, yp, zm, zp = ws
        step = 1 << level
        x = xm.shape[0] // Y
        rows, lanes = self.rows_of(x), self.lanes_of(x)
        diagonal = reaction + xm + xp + ym + yp + zm + zp
        zero = jnp.zeros_like(xm)
        w[DG] = diagonal
        w[INV] = 1.0 / diagonal
        w[XM] = xm
        w[XP] = xp
        w[YM] = jnp.where(rows < step, zero, ym)
        w[YP] = jnp.where(rows >= Y - step, zero, yp)
        w[ZM] = jnp.where(lanes < step, zero, zm)
        w[ZP] = jnp.where(lanes >= Z - step, zero, zp)
        if w.shape[0] > YB:
            w[YB] = jnp.where(rows < step, ym, jnp.where(rows >= Y - step, yp, zero))
            w[ZB] = jnp.where(lanes < step, zm, jnp.where(lanes >= Z - step, zp, zero))

    def inner(self, w, v, level):
        step = 1 << level
        acc = w[DG] * v
        acc = acc - w[YM] * roll(v, step, 0) - w[YP] * roll(v, -step, 0)
        acc = acc - w[ZM] * roll(v, step, 1) - w[ZP] * roll(v, -step, 1)
        Y = self.Y
        if v.shape[0] > Y:
            none = jnp.zeros((Y, self.Z), jnp.float32)
            acc = acc - w[XM] * cat([none, v[:-Y]]) - w[XP] * cat([v[Y:], none])
        return acc


def cat(parts):
    return parts[0] if len(parts) == 1 else jnp.concatenate(parts, axis=0)


def roll(v, shift, axis):
    return pltpu.roll(v, shift % v.shape[axis], axis)


def dot(a, b):
    return lax.dot_general(
        a, b, (((1,), (0,)), ((), ())), precision=lax.Precision.HIGHEST, preferred_element_type=jnp.float32
    )


def kernel(
    sizes, counts, tp_ref, it_ref, src_ref, rea_ref, dir_ref, rem_ref, le_ref, en_ref,
    sx, rx, sy, ry, sz, rz, ssem, rsem, lev0, lev1, glev2, glev3, p_ref, q_ref,
    phx, phy, phz, dhx, dhy, dhz, dot_all, en_all, red_ssem, red_rsem,
    picked, gat_pl, gat_x, set_pl, set_x, glob,
):
    X, Y, Z = sizes
    nx, ny, nz = counts
    planes = ny * nz
    levs = (lev0, lev1)
    L = len(levs)
    x_own, y_own, z_own = X >> L, Y >> L, Z >> L
    GY, GZ = ny * y_own, nz * z_own
    here, world = Grid(Y, Z), Grid(GY, GZ)
    rows_of, lanes_of = here.rows_of, here.lanes_of
    ix, iy, iz = lax.axis_index("gx"), lax.axis_index("gy"), lax.axis_index("gz")
    has = (ix > 0, ix < nx - 1, iy > 0, iy < ny - 1, iz > 0, iz < nz - 1)
    devs = (
        (ix - 1, iy, iz), (ix + 1, iy, iz), (ix, iy - 1, iz),
        (ix, iy + 1, iz), (ix, iy, iz - 1), (ix, iy, iz + 1),
    )
    send = (sx, sx, sy, sy, sz, sz)
    recv = (rx, rx, ry, ry, rz, rz)
    lane_y = lax.broadcasted_iota(jnp.int32, (Y, Z), 1)
    lane_1 = lax.broadcasted_iota(jnp.int32, (1, Z), 1)

    for d in range(6):
        @pl.when(jnp.logical_not(has[d]))
        def _():
            recv[d][:, d % 2] = jnp.zeros(recv[d].shape[:1] + recv[d].shape[2:], jnp.float32)

    def outgoing(d, slot):
        side = d % 2
        return pltpu.make_async_remote_copy(
            src_ref=send[d].at[slot, side],
            dst_ref=recv[d].at[slot, 1 - side],
            send_sem=ssem.at[slot, d],
            recv_sem=rsem.at[slot, d + 1 - 2 * side],
            device_id=devs[d],
            device_id_type=MESH,
        )

    def incoming(d, slot):
        side = d % 2
        return pltpu.make_async_remote_copy(
            src_ref=send[d].at[slot, side],
            dst_ref=recv[d].at[slot, side],
            send_sem=ssem.at[slot, d],
            recv_sem=rsem.at[slot, d],
            device_id=devs[d],
            device_id_type=MESH,
        )

    def go(d, slot):
        @pl.when(has[d])
        def _():
            outgoing(d, slot).start()

    def start(v, slot):
        x = v.shape[0] // Y
        sx[slot, 0] = v[:Y]
        sx[slot, 1] = v[-Y:]
        go(0, slot)
        go(1, slot)
        for i in range(x):
            sy[slot, 0, i : i + 1] = v[i * Y : i * Y + 1]
            sy[slot, 1, i : i + 1] = v[i * Y + Y - 1 : i * Y + Y]
        go(2, slot)
        go(3, slot)
        for side, lane in ((0, 0), (1, Z - 1)):
            packed = jnp.broadcast_to(v[:Y, lane : lane + 1], (Y, Z))
            for i in range(1, x):
                part = jnp.broadcast_to(v[i * Y : i * Y + Y, lane : lane + 1], (Y, Z))
                packed = jnp.where(lane_y == i, part, packed)
            sz[slot, side] = packed
        go(4, slot)
        go(5, slot)

    def finish(slot):
        for d in range(6):
            @pl.when(has[d])
            def _():
                copy = incoming(d, slot)
                copy.wait_recv()
                copy.wait_send()

    def wide_y(half, x):
        return cat([jnp.broadcast_to(half[i : i + 1], (Y, Z)) for i in range(x)])

    def wide_z(half, x):
        return cat([jnp.broadcast_to(half[:, i : i + 1], (Y, Z)) for i in range(x)])

    def beyond(w, acc, in_x0, in_x1, in_y, in_z):
        x = acc.shape[0] // Y
        acc = acc - w[YB] * in_y - w[ZB] * in_z
        low = w[XM, :Y] * in_x0
        high = w[XP, (x - 1) * Y :] * in_x1
        if x == 1:
            return acc - low - high
        return cat([acc[:Y] - low] + ([acc[Y:-Y]] if x > 2 else []) + [acc[-Y:] - high])

    def operate(v, level, slot):
        w = levs[level]
        x = X >> level
        start(v, slot)
        acc = here.inner(w, v, level)
        finish(slot)
        in_y = jnp.where(rows_of(x) < Y // 2, wide_y(ry[slot, 0], x), wide_y(ry[slot, 1], x))
        in_z = jnp.where(lanes_of(x) < Z // 2, wide_z(rz[slot, 0], x), wide_z(rz[slot, 1], x))
        return beyond(w, acc, rx[slot, 0], rx[slot, 1], in_y, in_z)

    turn = [0]

    def apply(v, level):
        slot = turn[0] % ROUND
        turn[0] += 1
        return operate(v, level, slot)

    def vcycle(r, level, part):
        w = levs[level]
        u = w[INV] * r * (1.0 / MID)
        total = u
        r = r - apply(u, level)
        u = RHO1 * RHO0 * u + 2.0 * RHO1 / HALF * w[INV] * r
        total = total + u
        r = r - apply(u, level)
        coarse = here.restrict(r, level)
        if level + 1 < L:
            e = here.prolong(vcycle(coarse, level + 1, part))
            r = r - apply(e, level)
        else:
            everywhere = collect(coarse, 1, part, gat_pl, gat_x, 4)
            e, ends = spread(world_cycle(everywhere[0], level + 1))
            r = r - beyond(w, here.inner(w, e, level), *ends)
        total = total + e
        u = w[INV] * r * (1.0 / MID)
        total = total + u
        r = r - apply(u, level)
        u = RHO1 * RHO0 * u + 2.0 * RHO1 / HALF * w[INV] * r
        return total + u

    def world_cycle(r, level):
        w = (glev2, glev3)[level - L]

        def apply(v):
            return world.inner(w, v, level - L)

        u = w[INV] * r * (1.0 / MID)
        total = u
        r = r - apply(u)
        u = RHO1 * RHO0 * u + 2.0 * RHO1 / HALF * w[INV] * r
        total = total + u
        r = r - apply(u)
        if level == LEVELS - 1:
            u = RHO2 * RHO1 * u + 2.0 * RHO2 / HALF * w[INV] * r
            return total + u
        e = world.prolong(world_cycle(world.restrict(r, level - L), level + 1))
        total = total + e
        r = r - apply(e)
        u = w[INV] * r * (1.0 / MID)
        total = total + u
        r = r - apply(u)
        u = RHO1 * RHO0 * u + 2.0 * RHO1 / HALF * w[INV] * r
        return total + u

    def hot(shape, wanted):
        at = lax.broadcasted_iota(jnp.int32, shape, 0)
        return jnp.where(at == wanted, 1.0, 0.0)

    def collect(v, fields, part, pl_ref, x_ref, which):
        count = fields * x_own * y_own
        picked[: fields * x_own * Y] = v
        own = picked[pl.ds(0, count, stride=1 << L), :]
        lane = lax.broadcasted_iota(jnp.int32, (Z, GZ), 1) - iz * z_own
        inside = jnp.logical_and(lane >= 0, lane < z_own)
        put = hot((Z, GZ), jnp.where(inside, lane * (1 << L), -1))
        pl_ref[part, my_plane] = dot(own, put)
        gather(pl_ref, part, planes, my_plane, in_plane, which)
        for j in range(ny):
            rows = pl_ref[part, j * nz]
            for k in range(1, nz):
                rows = rows + pl_ref[part, j * nz + k]
            for i in range(fields * x_own):
                x_ref[part, ix, i * GY + j * y_own : i * GY + (j + 1) * y_own] = rows[i * y_own : (i + 1) * y_own]
        gather(x_ref, part, nx, ix, in_column, which + 1)
        return [
            cat([x_ref[part, d, f * x_own * GY : (f + 1) * x_own * GY] for d in range(nx)]) for f in range(fields)
        ]

    def spread(v):
        lane = lax.broadcasted_iota(jnp.int32, (GZ, Z), 1)
        inside = hot((GZ, Z), iz * z_own + lane // (1 << L))
        outside = hot((GZ, Z), jnp.where(lane < Z // 2, iz * z_own - 1, iz * z_own + z_own))
        glob[0, GY : GY + nx * x_own * GY] = dot(v, inside)
        glob[1, GY : GY + nx * x_own * GY] = dot(v, outside)
        rows = rows_of(1)

        def layer(which, a):
            base = (ix * x_own + 1 + a) * GY + iy * y_own
            out = jnp.broadcast_to(glob[which, pl.ds(base, 1), :], (Y, Z))
            for j in range(1, y_own):
                row = jnp.broadcast_to(glob[which, pl.ds(base + j, 1), :], (Y, Z))
                out = jnp.where(rows < j << L, out, row)
            return out

        def rims(a):
            base = (ix * x_own + 1 + a) * GY + iy * y_own
            low = glob[0, pl.ds(base - 1, 1), :] * has_low
            high = glob[0, pl.ds(base + y_own, 1), :] * has_high
            return jnp.where(rows < Y // 2, jnp.broadcast_to(low, (Y, Z)), jnp.broadcast_to(high, (Y, Z)))

        has_low = jnp.where(iy > 0, 1.0, 0.0)
        has_high = jnp.where(iy < ny - 1, 1.0, 0.0)
        own = range(x_own)
        e = here.prolong(cat([layer(0, a) for a in own]))
        in_y = here.prolong(cat([rims(a) for a in own]))
        in_z = here.prolong(cat([layer(1, a) for a in own]))
        return e, (layer(0, -1), layer(0, x_own), in_y, in_z)

    def gather(ref, part, count, me, device, which):
        for j in range(count):
            @pl.when(me != j)
            def _():
                pltpu.make_async_remote_copy(
                    src_ref=ref.at[part, me],
                    dst_ref=ref.at[part, me],
                    send_sem=red_ssem.at[which, part],
                    recv_sem=red_rsem.at[which, part],
                    device_id=device(j),
                    device_id_type=MESH,
                ).start()
        if count > 1:
            others = ref.at[part, pl.ds(0, count - 1)]
            pltpu.make_async_copy(others, others, red_rsem.at[which, part]).wait()
            pltpu.make_async_copy(others, others, red_ssem.at[which, part]).wait()

    def in_plane(j):
        return (ix, j // nz, j % nz)

    def in_column(j):
        return (j, iy, iz)

    def in_grid(j):
        return (j // planes, j // nz % ny, j % nz)

    my_plane = iy * nz + iz
    me = ix * planes + my_plane

    def reduce_plane(ref, part, value, which):
        ref[part, my_plane] = value
        gather(ref, part, planes, my_plane, in_plane, which)
        return jnp.sum(ref[part], axis=0)

    def reduce_column(ref, part, value, which):
        ref[part, ix] = value
        gather(ref, part, nx, ix, in_column, which)
        return jnp.sum(ref[part], axis=0)

    def total_of(v):
        return jnp.sum(jnp.sum(v, axis=0, keepdims=True), axis=1, keepdims=True)

    def lane_of(row, i):
        return jnp.sum(jnp.where(lane_1 == i, row, 0.0), axis=1, keepdims=True)

    it = it_ref[...].reshape(X * Y, Z)
    reaction = rea_ref[...].reshape(X * Y, Z)
    start(it, KEPT)
    finish(KEPT)
    rows, lanes = rows_of(X), lanes_of(X)
    last_row, last_lane = rows == Y - 1, lanes == Z - 1
    n_xm = cat([rx[KEPT, 0], it[:-Y]])
    n_xp = cat([it[Y:], rx[KEPT, 1]])
    n_ym = jnp.where(rows == 0, wide_y(ry[KEPT, 0], X), roll(it, 1, 0))
    n_yp = jnp.where(last_row, wide_y(ry[KEPT, 1], X), roll(it, -1, 0))
    n_zm = jnp.where(lanes == 0, wide_z(rz[KEPT, 0], X), roll(it, 1, 1))
    n_zp = jnp.where(last_lane, wide_z(rz[KEPT, 1], X), roll(it, -1, 1))
    ws = []
    r = src_ref[...].reshape(X * Y, Z) - reaction * it
    for sign, n in ((-1, n_xm), (1, n_xp), (-1, n_ym), (1, n_yp), (-1, n_zm), (1, n_zp)):
        g = n - it
        square = g * g
        root = jnp.sqrt(1.0 + square)
        ws.append((1.0 + 2.0 * square) / root)
        r = r + g * root
    rem_ref[...] = r.reshape(X, Y, Z)
    here.put(levs[0], 0, ws, reaction)
    for level in range(L):
        ws, reaction = here.coarsen(ws, reaction, level)
        if level + 1 < L:
            here.put(levs[level + 1], level + 1, ws, reaction)
    glob[...] = jnp.zeros_like(glob)
    *ws, reaction = collect(cat(list(ws) + [reaction]), 7, 0, set_pl, set_x, 6)
    world.put(glev2, 0, ws, reaction)
    world.put(glev3, 1, *world.coarsen(ws, reaction, 0))
    for ref in (p_ref, q_ref, phx, phy, phz, dhx, dhy, dhz):
        ref[...] = jnp.zeros_like(ref)
    dir_ref[...] = jnp.zeros_like(dir_ref)

    def body(it_idx, carry):
        rz_old, pq_old = carry
        part = lax.rem(it_idx, 2)
        r = rem_ref[...].reshape(X * Y, Z)
        turn[0] = 0
        z = vcycle(r, 0, part)
        z_slot = turn[0] % ROUND
        az = apply(z, 0)
        q_old = q_ref[...]
        sums = jnp.where(
            lane_1 == 0,
            total_of(rem_ref[...].reshape(X * Y, Z) * z),
            jnp.where(lane_1 == 1, total_of(z * az), total_of(z * q_old)),
        )
        dot_all[part, me] = sums
        gather(dot_all, part, nx * planes, me, in_grid, 0)
        row = jnp.sum(dot_all[part], axis=0)
        rz_new, zaz, zq = lane_of(row, 0), lane_of(row, 1), lane_of(row, 2)
        beta = rz_new / rz_old
        pq = zaz + 2.0 * beta * zq + beta * beta * pq_old
        a = rz_new / pq
        p = z + beta * p_ref[...]
        q = az + beta * q_old
        p_ref[...] = p
        q_ref[...] = q
        dir_ref[...] = dir_ref[...] + (a * p).reshape(X, Y, Z)
        rem_ref[...] = rem_ref[...] - (a * q).reshape(X, Y, Z)
        for got, ph, dh in ((rx, phx, dhx), (ry, phy, dhy), (rz, phz, dhz)):
            for side in range(2):
                edge = got[z_slot, side] + beta * ph[side]
                ph[side] = edge
                dh[side] = dh[side] + a * edge
        return rz_new, pq

    one = jnp.ones((1, 1), jnp.float32)
    lax.fori_loop(0, ITERS, body, (one, jnp.zeros((1, 1), jnp.float32)))

    it = it_ref[...].reshape(X * Y, Z)
    step_dir = dir_ref[...].reshape(X * Y, Z)

    def energy(g):
        square = 1.0 + g * g
        return (square * jnp.sqrt(square) - 1.0) * (1.0 / 3.0)

    ends_y = jnp.where(jnp.logical_and(last_row, iy == ny - 1), 1.0, 0.0)
    ends_z = jnp.where(jnp.logical_and(last_lane, iz == nz - 1), 1.0, 0.0)
    ends_x = jnp.where(ix == nx - 1, 1.0, 0.0)
    across = lax.broadcasted_iota(jnp.int32, (X, Z), 0) == lax.broadcasted_iota(jnp.int32, (X, Z), 1)
    trial_rows = []
    for k in range(TRIALS):
        s = jnp.exp2(-jnp.full((1, Z), tp_ref[k], jnp.int32).astype(jnp.float32))
        v = it + s * step_dir
        low_x = cat([rx[KEPT, 0] + s * dhx[0], v[:-Y]])
        low_y = jnp.where(rows == 0, wide_y(ry[KEPT, 0] + s * dhy[0], X), roll(v, 1, 0))
        low_z = jnp.where(lanes == 0, wide_z(rz[KEPT, 0] + s * dhz[0], X), roll(v, 1, 1))
        at_end = energy(v)
        e = energy(v - low_x) + energy(v - low_y) + energy(v - low_z)
        e = e + at_end * (ends_y + ends_z)
        e = cat([e[:-Y], e[-Y:] + ends_x * at_end[-Y:]]) if X > 1 else e + ends_x * at_end
        e = e + 0.5 * rea_ref[...].reshape(X * Y, Z) * v * v - src_ref[...].reshape(X * Y, Z) * v
        by_layer = jnp.sum(jnp.sum(e.reshape(X, Y, Z), axis=1), axis=1, keepdims=True)
        trial_rows.append(jnp.sum(jnp.where(across, by_layer, 0.0), axis=0, keepdims=True))
    en_all[0, me] = jnp.concatenate(trial_rows, axis=0)
    gather(en_all, 0, nx * planes, me, in_grid, 2)
    layers = jnp.sum(en_all[0, pl.ds(ix * planes, planes)], axis=0)
    layers = layers / (Y * ny * Z * nz)
    le_ref[...] = layers[:, :X]
    overall = jnp.sum(en_all[0], axis=0) / (Y * ny * Z * nz)
    overall = jnp.sum(overall, axis=1, keepdims=True) / (X * nx)
    en_ref[...] = jnp.broadcast_to(overall, (TRIALS, Z))


def on_device(counts, iterate, source, reaction, trial_powers):
    X, Y, Z = iterate.shape
    nx, ny, nz = counts
    f32 = jnp.float32
    slots = ROUND + 1
    vm = pltpu.VMEM
    scratch = [vm((slots, 2, rows, Z), f32) for rows in (Y, Y, X, X, Y, Y)]
    scratch += [pltpu.SemaphoreType.DMA((slots, 6))] * 2
    x_own, y_own = X // 4, Y // 4
    GX, GY, GZ = nx * x_own, ny * y_own, nz * Z // 4
    scratch += [vm((10, (X >> level) * Y, Z), f32) for level in range(2)]
    scratch += [vm((8, (GX >> level) * GY, GZ), f32) for level in range(2)]
    scratch += [vm((X * Y, Z), f32)] * 2
    scratch += [vm((2, rows, Z), f32) for rows in (Y, X, Y)] * 2
    scratch += [
        vm((2, nx * ny * nz, 1, Z), f32),
        vm((1, nx * ny * nz, TRIALS, Z), f32),
        pltpu.SemaphoreType.DMA((8, 2)), pltpu.SemaphoreType.DMA((8, 2)),
        vm((7 * x_own * Y, Z), f32),
        vm((2, ny * nz, x_own * y_own, GZ), f32), vm((2, nx, x_own * GY, GZ), f32),
        vm((1, ny * nz, 7 * x_own * y_own, GZ), f32), vm((1, nx, 7 * x_own * GY, GZ), f32),
        vm((2, (GX + 2) * GY, Z), f32),
    ]
    whole = pl.BlockSpec(memory_space=pltpu.VMEM)
    out = pl.pallas_call(
        functools.partial(kernel, (X, Y, Z), counts),
        out_shape=[
            jax.ShapeDtypeStruct((X, Y, Z), f32),
            jax.ShapeDtypeStruct((X, Y, Z), f32),
            jax.ShapeDtypeStruct((TRIALS, X), f32),
            jax.ShapeDtypeStruct((TRIALS, Z), f32),
        ],
        in_specs=[pl.BlockSpec(memory_space=pltpu.SMEM), whole, whole, whole],
        out_specs=[whole] * 4,
        scratch_shapes=scratch,
        compiler_params=pltpu.CompilerParams(has_side_effects=True, vmem_limit_bytes=48 * 1024 * 1024),
        name="newton_step",
    )(trial_powers, iterate, source, reaction)
    return out[0], out[1], out[2], out[3][:, 0]


def solution(mesh):
    counts = tuple(mesh.shape[axis] for axis in ("gx", "gy", "gz"))
    grid = P("gx", "gy", "gz")
    return jax.shard_map(
        functools.partial(on_device, counts),
        mesh=mesh,
        in_specs=(grid, grid, grid, P()),
        out_specs=(grid, grid, P(None, "gx"), P()),
        check_vma=False,
    )
```
